32 devices in a mesh: slab: 8 (over z, core), sub: 4 (over y, x).
Axes of the slice: x: 2, y: 2, z: 4, core: 2. Of those that a mesh axis runs over, the one named last changes fastest.
Arguments:
- child_moments: bfloat16 [216, 32768], P(None, ('slab', 'sub')), may hold values from -6 to 6
- incoming: bfloat16 [216, 4096], P(None, ('slab', 'sub')), may hold values from -6 to 6
- m2m_ops: bfloat16 [8, 216, 216], replicated, may hold values from -0.15625 to 0.15625
- m2l_ops: bfloat16 [160, 216, 216], P('sub'), may hold values from -0.046875 to 0.046875
- l2l_ops: bfloat16 [8, 216, 216], replicated, may hold values from -0.4375 to 0.4375
- partners: int32 [160, 4096], P(None, ('slab', 'sub')), may hold values from -1 to 4095, as said below
Outputs:
- child_locals: float32 [216, 32768], P(None, ('slab', 'sub'))
The draws below stay inside these ranges and needn't reach their ends.
Inputs may be any that keep to these rules, and one draw needn't show every extreme that they name: `partners`: cells are numbered in Morton order of bricks of the domain, each brick one cell wide along the first dimension; the source of a pair lies in the same slab as its target or in an adjacent one, that is its id divided by 128 * 4 differs from the target's by at most one. Pairs are those of the interaction list: source and target are not adjacent, their parents are.
All inputs are finite; a program needn't handle non-finite values.
Results may differ from the reference program's by a relative error of at most 0.0035.
Values may be sent and summed in bfloat16 or wider, within the bound.
No kernel may reach another device: no remote copies, remote signals or barrier semaphores. Data moves between devices by JAX's collectives and lax.ppermute only.
A program may use at most 128 MiB of HBM per device.

```python
import math
import jax
import jax.numpy as jnp
import numpy as np
from jax import lax

W = 216
OPS = 160
CELLS_DEV = 128
CELLS = 4096
LEAVES = 32768
N_SLAB = 8
N_SUB = 4


def offset_rows():
    forced = [(2, 0, 0), (-2, 0, 0), (1, 0, 2), (-1, 0, 2)]
    entries = list(forced)
    for first in range(-3, 4):
        for second in range(-3, 4):
            for third in range(-3, 4):
                if max(abs(first), abs(second), abs(third)) > 1 and (first, second, third) not in forced:
                    entries.append((first, second, third))
    return np.array(entries, np.int32)


def draw_partners(key, part):
    table_all = jnp.asarray(offset_rows())
    rest_count = table_all.shape[0] - 4
    chosen = jnp.concatenate([jnp.arange(4, dtype=jnp.int32), 4 + jax.random.permutation(key, rest_count)[:OPS - 4].astype(jnp.int32)])
    shifts = table_all[chosen]
    side_x = math.isqrt(N_SUB)
    side_y = N_SUB // side_x
    brick_depth = CELLS_DEV // 16
    cell_total = CELLS_DEV * N_SLAB * N_SUB
    cell_ids = jnp.arange(cell_total, dtype=jnp.int32)
    device_ids = cell_ids // CELLS_DEV
    inner_ids = cell_ids % CELLS_DEV
    slab_ids = device_ids // N_SUB
    sub_ids = device_ids % N_SUB
    pos_x = sub_ids // side_y
    pos_y = sub_ids % side_y * 16 + inner_ids % 2 + 2 * (inner_ids // 2 % 2) + 4 * (inner_ids // 8 % 2) + 8 * (inner_ids // 16 % 2)
    pos_z = slab_ids * brick_depth + inner_ids // 4 % 2 + 2 * (inner_ids // 32 % 2) + 4 * (inner_ids // 64)
    far_x = pos_x[None, :] + shifts[:, 0:1]
    far_y = pos_y[None, :] + shifts[:, 1:2]
    far_z = pos_z[None, :] + shifts[:, 2:3]
    inside = (far_x >= 0) & (far_x < side_x) & (far_y >= 0) & (far_y < 16 * side_y)
    inside = inside & (far_z >= 0) & (far_z < brick_depth * N_SLAB)
    near = jnp.abs(jnp.floor_divide(far_x, 2) - pos_x[None, :] // 2) <= 1
    near = near & (jnp.abs(jnp.floor_divide(far_y, 2) - pos_y[None, :] // 2) <= 1)
    near = near & (jnp.abs(jnp.floor_divide(far_z, 2) - pos_z[None, :] // 2) <= 1)
    safe_x = jnp.clip(far_x, 0, side_x - 1)
    safe_y = jnp.clip(far_y, 0, 16 * side_y - 1)
    safe_z = jnp.clip(far_z, 0, brick_depth * N_SLAB - 1)
    loc_y = safe_y % 16
    loc_z = safe_z % brick_depth
    inner_new = loc_y % 2 + 2 * (loc_y // 2 % 2) + 4 * (loc_z % 2) + 8 * (loc_y // 4 % 2) + 16 * (loc_y // 8 % 2)
    inner_new = inner_new + 32 * (loc_z // 2 % 2) + 64 * (loc_z // 4)
    device_new = safe_z // brick_depth * N_SUB + safe_x * side_y + safe_y // 16
    source_ids = device_new * CELLS_DEV + inner_new
    return jnp.where(inside & near, source_ids, -1).astype(jnp.int32)


def block_levels(stream_key, shape, split, least, top_value):
    level = 1.0
    for axis_at, blocks in split:
        draws = jax.random.uniform(jax.random.fold_in(jax.random.fold_in(stream_key, 6), axis_at), (blocks,), jnp.float32, least / len(split), top_value / len(split))
        level = level * jnp.repeat(jnp.exp(draws), shape[axis_at] // blocks).reshape((-1,) + (1,) * (len(shape) - 1 - axis_at))
    return level


def gaussian(key, dims, width, reach, shards=(), held_as=jnp.bfloat16):
    result = jax.random.normal(key, dims, jnp.float32) * width
    if len(shards) > 0:
        result = block_levels(key, dims, shards, -0.22, 0.18) * result
    return jnp.clip(result, min=-reach, max=reach).astype(held_as)


def setup_inputs(seed: int = 0) -> dict:
    streams_of = jax.random.split(jax.random.key(seed), 7)
    return {
        "child_moments": gaussian(streams_of[0], (W, LEAVES), 1.0, 6.0, ((1, 32),)),
        "incoming": gaussian(streams_of[1], (W, CELLS), 1.0, 6.0, ((1, 32),)),
        "m2m_ops": gaussian(streams_of[2], (8, W, W), (8 * W) ** -0.5, 0.15625),
        "m2l_ops": gaussian(streams_of[3], (OPS, W, W), (W * OPS // 2) ** -0.5, 0.046875, ((0, 4),)),
        "l2l_ops": gaussian(streams_of[4], (8, W, W), W ** -0.5, 0.4375),
        "partners": draw_partners(jax.random.fold_in(streams_of[6], 71), 0),
    }


def reference(child_moments, incoming, m2m_ops, m2l_ops, l2l_ops, partners):
    order_cube = child_moments.shape[0]
    cell_count = child_moments.shape[1] // 8
    children = child_moments.astype(jnp.float32).reshape(order_cube, cell_count, 8)
    moments = jnp.einsum("oij,jpo->ip", m2m_ops.astype(jnp.float32), children).astype(jnp.bfloat16)

    def apply_op(summed, operand_pair):
        op_matrix, source_row = operand_pair
        usable = source_row >= 0
        columns = jnp.take(moments, jnp.where(usable, source_row, 0).astype(jnp.int32), axis=1)
        columns = jnp.where(usable[None, :], columns, jnp.zeros((), jnp.bfloat16))
        return summed + jnp.dot(op_matrix, columns, preferred_element_type=jnp.float32), None

    far_field, _ = lax.scan(apply_op, jnp.zeros((order_cube, cell_count), jnp.float32), (m2l_ops, partners))
    locals_all = (incoming.astype(jnp.float32) + far_field).astype(jnp.bfloat16)
    child_out = jnp.einsum("oij,jp->ipo", l2l_ops.astype(jnp.float32), locals_all.astype(jnp.float32))
    return child_out.reshape(order_cube, cell_count * 8)
```

```python
import functools

import jax
import jax.numpy as jnp
from jax import lax
from jax.experimental import pallas as pl
from jax.experimental.pallas import tpu as pltpu
from jax.sharding import PartitionSpec as P

RIM = 32
TILE = 256


def peer(r, i, n):
    return i ^ r if n & (n - 1) == 0 else (r - i) % n


def slot_of(i, j, n):
    return i ^ j if n & (n - 1) == 0 else (i + j) % n


def swap(x, r, n):
    if r == 0 and n & (n - 1) == 0:
        return x
    return lax.ppermute(x, "sub", [(i, peer(r, i, n)) for i in range(n)])


def m2l_kernel(n_sub, flags, idx, *refs):
    own = refs[:n_sub]
    rims = refs[n_sub : 2 * n_sub]
    ops = refs[2 * n_sub]
    outs = refs[2 * n_sub + 1 : 3 * n_sub + 1]
    win, acc, cols, todo = refs[3 * n_sub + 1 :]
    order, cells = own[0].shape
    n_ops = ops.shape[0]
    tiles = acc.shape[0]
    units = n_ops * tiles
    per_tile = TILE // cells
    span = win.shape[1]
    rim_base = n_sub * cells
    rim_cols = rims[0].shape[1]

    def scan(u, count):
        todo[count] = u
        return count + flags[u]

    count = lax.fori_loop(0, units, scan, 0)
    todo[count] = units
    todo[count + 1] = units
    trips = (count + 1) // 2

    for r in range(n_sub):
        win[:, r * cells : (r + 1) * cells] = own[r][...]
    per_block = cells // rim_cols
    for b in range(n_sub * rim_cols // cells):
        parts = [rims[b * per_block + q][...] for q in range(per_block)]
        win[:, rim_base + b * cells : rim_base + (b + 1) * cells] = jnp.concatenate(parts, axis=1)
    acc[...] = jnp.zeros_like(acc)
    cols[...] = jnp.zeros_like(cols)

    def pick(u):
        row = idx[u]
        total = None
        for t in range(span // TILE):
            rel = (row - float(t * TILE)).astype(jnp.bfloat16)
            rows = lax.broadcasted_iota(jnp.int32, (TILE, TILE), 0).astype(jnp.float32).astype(jnp.bfloat16)
            hot = jnp.where(rows == jnp.broadcast_to(rel, (TILE, TILE)), 1.0, 0.0).astype(jnp.bfloat16)
            part = jnp.dot(win[:, t * TILE : (t + 1) * TILE], hot, preferred_element_type=jnp.float32)
            total = part if total is None else total + part
        return total.astype(jnp.bfloat16)

    def body(i, carry):
        slot = lax.rem(i, 2)
        prev = 1 - slot
        fresh = [pick(todo[jnp.minimum(2 * i + a, count)]) for a in range(2)]
        for a in range(2):
            u = todo[jnp.clip(2 * i - 2 + a, 0, count)]
            k = jnp.minimum(u // tiles, n_ops - 1)
            acc[lax.rem(u, tiles)] += jnp.dot(
                ops[k], cols[2 * prev + a], preferred_element_type=jnp.float32
            )
        for a in range(2):
            cols[2 * slot + a] = fresh[a]
        return carry

    lax.fori_loop(0, trips + 1, body, 0)
    for r in range(n_sub):
        part = acc[r // per_tile, :, (r % per_tile) * cells : (r % per_tile + 1) * cells]
        outs[r][...] = part.astype(outs[r].dtype)


def m2l(flags, idx, own, rims, ops):
    n_sub = len(own)
    order, cells = own[0].shape
    n_ops = ops.shape[0]
    span = n_sub * (cells + rims[0].shape[1])
    tiles = n_sub * cells // TILE
    units = n_ops * tiles
    vmem = pl.BlockSpec(memory_space=pltpu.VMEM)
    return pl.pallas_call(
        functools.partial(m2l_kernel, n_sub),
        out_shape=[jax.ShapeDtypeStruct((order, cells), jnp.float32)] * n_sub,
        in_specs=[pl.BlockSpec(memory_space=pltpu.SMEM)] + [vmem] * (2 * n_sub + 2),
        out_specs=[vmem] * n_sub,
        scratch_shapes=[
            pltpu.VMEM((order, span), jnp.bfloat16),
            pltpu.VMEM((tiles, order, TILE), jnp.float32),
            pltpu.VMEM((4, order, TILE), jnp.bfloat16),
            pltpu.SMEM((units + 2,), jnp.int32),
        ],
        cost_estimate=pl.CostEstimate(flops=2 * units * order * TILE * span, bytes_accessed=8 << 20, transcendentals=0),
        name="m2l",
    )(flags, idx, *own, *rims, ops)


def local(child_moments, incoming, m2m_ops, m2l_ops, l2l_ops, partners):
    order = child_moments.shape[0]
    cells = child_moments.shape[1] // 8
    n_sub = lax.axis_size("sub")
    n_slab = lax.axis_size("slab")
    me = lax.axis_index("sub")
    my_slab = lax.axis_index("slab")
    n_ops = m2l_ops.shape[0]

    source = partners // cells
    inner = partners % cells
    delta = source // n_sub - my_slab
    holder = (jnp.arange(partners.shape[0], dtype=jnp.int32) // n_ops)[:, None]
    block = slot_of(holder, source % n_sub, n_sub)
    rim_at = n_sub * cells + block * (2 * RIM)
    column = jnp.where(
        delta == 0,
        block * cells + inner,
        jnp.where(delta < 0, rim_at + inner - (cells - RIM), rim_at + inner + RIM),
    )
    column = jnp.where(partners >= 0, column, -1).reshape(n_sub, n_ops, cells)
    lists = [swap(column[peer(r, me, n_sub)], r, n_sub) for r in range(n_sub)]
    tiles = n_sub * cells // TILE
    idx = jnp.concatenate(lists, axis=1).reshape(n_ops * tiles, 1, TILE)
    flags = jnp.any(idx >= 0, axis=(1, 2)).astype(jnp.int32)
    idx = jnp.concatenate([idx, jnp.full((1, 1, TILE), -1, idx.dtype)], axis=0).astype(jnp.float32)

    children = child_moments.reshape(order, cells, 8)
    moments = jnp.einsum("oij,jpo->ip", m2m_ops, children, preferred_element_type=jnp.float32).astype(jnp.bfloat16)
    up = [(i, i + 1) for i in range(n_slab - 1)]
    below = lax.ppermute(moments[:, cells - RIM :], "slab", up)
    above = lax.ppermute(moments[:, :RIM], "slab", [(b, a) for a, b in up])
    rim = jnp.concatenate([below, above], axis=1)
    own = [swap(moments, r, n_sub) for r in range(n_sub)]
    rims = [swap(rim, r, n_sub) for r in range(n_sub)]

    parts = m2l(flags, idx, own, rims, m2l_ops)
    back = [swap(parts[r], r, n_sub) for r in range(n_sub)]
    far = functools.reduce(lambda a, b: a + b, back)
    locals_all = (incoming.astype(jnp.float32) + far).astype(jnp.bfloat16)
    child_out = jnp.einsum("oij,jp->ipo", l2l_ops, locals_all, preferred_element_type=jnp.float32)
    return child_out.reshape(order, cells * 8)


def solution(mesh):
    in_specs = (
        P(None, ("slab", "sub")),
        P(None, ("slab", "sub")),
        P(),
        P("sub", None, None),
        P(),
        P(None, ("slab", "sub")),
    )
    out_specs = P(None, ("slab", "sub"))
    return jax.shard_map(local, mesh=mesh, in_specs=in_specs, out_specs=out_specs, check_vma=False)
```

```python
import functools

import jax
import jax.numpy as jnp
from jax import lax
from jax.experimental import pallas as pl
from jax.experimental.pallas import tpu as pltpu
from jax.sharding import PartitionSpec as P

RIM = 32
TILE = 256
LANES = 128
GROUP = 4
VMEM = pl.BlockSpec(memory_space=pltpu.VMEM)
BF16 = jnp.bfloat16
F32 = jnp.float32


def peer(r, i, n):
    return i ^ r if n & (n - 1) == 0 else (r - i) % n


def slot_of(i, j, n):
    return i ^ j if n & (n - 1) == 0 else lax.rem(i + j, n)


def swap(x, r, n):
    if r == 0 and n & (n - 1) == 0:
        return x
    return lax.ppermute(x, "sub", [(i, peer(r, i, n)) for i in range(n)])


def half_rows(n_ops):
    return -(-n_ops // 16) * 16


def iota(shape, dim):
    return lax.broadcasted_iota(jnp.int32, shape, dim)


def up_kernel(n_sub, child, ops, partners, moments, codes):
    order, cells = moments.shape
    span = cells // 4
    lane = iota((1, TILE), 1)
    row = iota((TILE, TILE), 0).astype(F32).astype(BF16)
    total = None
    for a in range(4):
        want = 8 * (lane % cells) + 2 * a + lane // cells
        cols = None
        for q in range(8 * cells // TILE):
            rel = (want - q * TILE).astype(F32).astype(BF16)
            hot = jnp.where(row == jnp.broadcast_to(rel, (TILE, TILE)), 1.0, 0.0).astype(BF16)
            part = jnp.dot(child[:, q * TILE : (q + 1) * TILE], hot, preferred_element_type=F32)
            cols = part if cols is None else cols + part
        cols = cols.astype(BF16)
        for b in range(2):
            part = jnp.dot(ops[2 * a + b], cols[:, b * cells : (b + 1) * cells], preferred_element_type=F32)
            total = part if total is None else total + part
    moments[...] = total.astype(BF16)

    n_ops = partners.shape[0] // n_sub
    my_slab = lax.axis_index("slab")
    codes[...] = jnp.zeros_like(codes)
    stride = half_rows(n_ops)
    for q in range(n_sub):
        ids = partners[q * n_ops : (q + 1) * n_ops, :]
        safe = jnp.maximum(ids, 0)
        source = lax.div(safe, cells)
        inner = safe - source * cells
        slab = lax.div(source, n_sub)
        block = slot_of(source - slab * n_sub, q, n_sub)
        delta = slab - my_slab
        rim_at = n_sub * cells + block * (2 * RIM)
        column = jnp.where(
            delta == 0,
            block * cells + inner,
            jnp.where(delta < 0, rim_at + inner - (cells - RIM), rim_at + inner + RIM),
        )
        code = lax.shift_left(LANES + (column & (LANES - 1)), lax.shift_right_logical(column, 7))
        code = jnp.where(ids >= 0, code, 0).astype(F32)
        if stride > n_ops:
            code = jnp.concatenate([code, jnp.zeros((stride - n_ops, cells), F32)], axis=0)
        codes[q, 0:stride, :] = code[:, : cells // 2].astype(BF16)
        codes[q, stride : 2 * stride, :] = code[:, cells // 2 :].astype(BF16)


def up(child, ops, partners, n_sub):
    order = child.shape[0]
    cells = child.shape[1] // 8
    return pl.pallas_call(
        functools.partial(up_kernel, n_sub),
        out_shape=[
            jax.ShapeDtypeStruct((order, cells), BF16),
            jax.ShapeDtypeStruct((n_sub, order, cells // 2), BF16),
        ],
        in_specs=[VMEM] * 3,
        out_specs=[VMEM] * 2,
        compiler_params=pltpu.CompilerParams(vmem_limit_bytes=16 << 20),
        cost_estimate=pl.CostEstimate(flops=1 << 30, bytes_accessed=2 << 20, transcendentals=0),
        name="up",
    )(child, ops, partners)


def m2l_kernel(n_sub, *refs):
    loads = refs[:n_sub]
    ops = refs[n_sub]
    outs = refs[n_sub + 1 : 2 * n_sub + 1]
    win, idx, code0, acc, cols, todo, scale = refs[2 * n_sub + 1 :]
    order, cells = outs[0].shape
    n_ops = ops.shape[0]
    n_tiles = acc.shape[0]
    k_tiles = win.shape[0]
    own_tiles = n_sub * cells // TILE
    stride = half_rows(n_ops)
    half = cells // 2

    for r in range(n_sub):
        win[r * cells // TILE, :, r * cells % TILE : r * cells % TILE + cells] = loads[r][:, :cells]
    for b in range(n_sub // 2):
        pair = jnp.concatenate(
            [loads[2 * b][:, cells : cells + half], loads[2 * b + 1][:, cells : cells + half]], axis=1
        )
        at = b * cells
        win[own_tiles + at // TILE, :, at % TILE : at % TILE + cells] = pair
    rows = iota((TILE, LANES), 0)
    code0[...] = lax.shift_left(LANES + (rows & (LANES - 1)), lax.shift_right_logical(rows, 7)).astype(F32).astype(BF16)

    bits = lax.shift_left(1, iota((n_ops, 1), 0) & 31)
    words = {}
    for n in range(n_tiles):
        parts = []
        for r in range(n * TILE // cells, (n + 1) * TILE // cells):
            parts.append(loads[r][0:stride, cells + half :].astype(F32)[:n_ops])
            parts.append(loads[r][stride : 2 * stride, cells + half :].astype(F32)[:n_ops])
        table = jnp.concatenate(parts, axis=1)
        idx[n, 0:n_ops, :] = table
        idx[n, n_ops : n_ops + 8, :] = jnp.zeros((8, TILE), F32)
        for t in range(k_tiles):
            high = float(LANES) * 4.0 ** (t + 1)
            hit = jnp.where((table >= float(LANES) * 4.0**t) & (table < high), 1.0, 0.0)
            hit = jnp.max(hit, axis=1, keepdims=True)
            word = jnp.where(hit > 0.0, bits, 0)
            for w in range(-(-n_ops // 32)):
                words[n, t, w] = jnp.sum(word[32 * w : min(32 * w + 32, n_ops)])
    for t in range(k_tiles):
        scale[t] = jnp.float32(4.0**-t)

    count = jnp.int32(0)
    for w in range(-(-n_ops // 32)):

        def scan(k, count, w=w):
            for n in range(n_tiles):
                for t in range(k_tiles):
                    todo[count] = ((32 * w + k) * n_tiles + n) * k_tiles + t
                    count = count + (lax.shift_right_logical(words[n, t, w], k) & 1)
            return count

        count = lax.fori_loop(0, min(32, n_ops - 32 * w), scan, count)
    for a in range(GROUP):
        todo[count + a] = n_ops * n_tiles * k_tiles
    trips = lax.div(count + GROUP - 1, GROUP)

    acc[...] = jnp.zeros_like(acc)
    cols[...] = jnp.zeros_like(cols)

    def unit(position):
        u = todo[position]
        kn = lax.div(u, k_tiles)
        k = lax.div(kn, n_tiles)
        return k, kn - k * n_tiles, u - kn * k_tiles

    def body(i, carry):
        slot = i & 1
        prev = 1 - slot
        for a in range(GROUP):
            k, n, t = unit(jnp.minimum(GROUP * i + a, count))
            row = (idx[n, pl.ds(k, 1), :] * scale[t]).astype(BF16)
            base = code0[...]
            hot = jnp.concatenate(
                [
                    jnp.where(base == jnp.broadcast_to(row[:, c : c + LANES], (TILE, LANES)), 1.0, 0.0).astype(BF16)
                    for c in range(0, TILE, LANES)
                ],
                axis=1,
            )
            cols[slot, a] = jnp.dot(win[t], hot, preferred_element_type=F32).astype(BF16)
        for a in range(GROUP):
            k, n, t = unit(jnp.clip(GROUP * (i - 1) + a, 0, count))
            acc[n] += jnp.dot(ops[jnp.minimum(k, n_ops - 1)], cols[prev, a], preferred_element_type=F32)
        return carry

    lax.fori_loop(0, trips + 1, body, 0)
    for r in range(n_sub):
        outs[r][...] = acc[r * cells // TILE, :, r * cells % TILE : r * cells % TILE + cells].astype(outs[r].dtype)


def m2l(loads, ops, cells):
    n_sub = len(loads)
    order = loads[0].shape[0]
    n_ops = ops.shape[0]
    n_tiles = n_sub * cells // TILE
    k_tiles = n_tiles + n_sub * 2 * RIM // TILE
    units = n_ops * n_tiles * k_tiles
    return pl.pallas_call(
        functools.partial(m2l_kernel, n_sub),
        out_shape=[jax.ShapeDtypeStruct((order, cells), F32)] * n_sub,
        in_specs=[VMEM] * (n_sub + 1),
        out_specs=[VMEM] * n_sub,
        scratch_shapes=[
            pltpu.VMEM((k_tiles, order, TILE), BF16),
            pltpu.VMEM((n_tiles, n_ops + 8, TILE), F32),
            pltpu.VMEM((TILE, LANES), BF16),
            pltpu.VMEM((n_tiles, order, TILE), F32),
            pltpu.VMEM((2, GROUP, order, TILE), BF16),
            pltpu.SMEM((units + GROUP,), jnp.int32),
            pltpu.SMEM((k_tiles,), F32),
        ],
        compiler_params=pltpu.CompilerParams(vmem_limit_bytes=24 << 20),
        cost_estimate=pl.CostEstimate(flops=8 << 30, bytes_accessed=8 << 20, transcendentals=0),
        name="m2l",
    )(*loads, ops)


def down_kernel(n_sub, incoming, *refs):
    parts = refs[:n_sub]
    ops, out, stage, sem = refs[n_sub:]
    cells = incoming.shape[1]
    far = parts[0][...].astype(F32)
    for r in range(1, n_sub):
        far = far + parts[r][...].astype(F32)
    held = (incoming[...].astype(F32) + far).astype(BF16)
    lane = iota((1, TILE), 1)
    cell = iota((cells, TILE), 0)
    copies = []
    for q in range(8 * cells // TILE):
        hot = jnp.where(cell == jnp.broadcast_to(q * (TILE // 8) + lane // 8, (cells, TILE)), 1.0, 0.0).astype(BF16)
        spread = jnp.dot(held, hot, preferred_element_type=F32)
        total = None
        for o in range(8):
            one = jnp.where(lane % 8 == o, spread, 0.0).astype(BF16)
            part = jnp.dot(ops[o], one, preferred_element_type=F32)
            total = part if total is None else total + part
        stage[q] = total
        copy = pltpu.make_async_copy(stage.at[q], out.at[:, q * TILE : (q + 1) * TILE], sem.at[q])
        copy.start()
        copies.append(copy)
    for copy in copies:
        copy.wait()


def down(incoming, parts, ops):
    order, cells = incoming.shape
    n_sub = len(parts)
    chunks = 8 * cells // TILE
    return pl.pallas_call(
        functools.partial(down_kernel, n_sub),
        out_shape=jax.ShapeDtypeStruct((order, 8 * cells), F32),
        in_specs=[VMEM] * (n_sub + 2),
        out_specs=pl.BlockSpec(memory_space=pl.ANY),
        scratch_shapes=[pltpu.VMEM((chunks, order, TILE), F32), pltpu.SemaphoreType.DMA((chunks,))],
        compiler_params=pltpu.CompilerParams(vmem_limit_bytes=16 << 20),
        cost_estimate=pl.CostEstimate(flops=1 << 30, bytes_accessed=2 << 20, transcendentals=0),
        name="down",
    )(incoming, *parts, ops)


def local(child_moments, incoming, m2m_ops, m2l_ops, l2l_ops, partners):
    cells = incoming.shape[1]
    n_sub = lax.axis_size("sub")
    n_slab = lax.axis_size("slab")
    me = lax.axis_index("sub")
    moments, codes = up(child_moments, m2m_ops, partners, n_sub)
    forward = [(i, i + 1) for i in range(n_slab - 1)]
    below = lax.ppermute(moments[:, cells - RIM :], "slab", forward)
    above = lax.ppermute(moments[:, :RIM], "slab", [(b, a) for a, b in forward])
    loads = []
    for r in range(n_sub):
        code = lax.dynamic_index_in_dim(codes, peer(r, me, n_sub), 0, keepdims=False)
        loads.append(swap(jnp.concatenate([moments, below, above, code], axis=1), r, n_sub))
    parts = m2l(loads, m2l_ops, cells)
    back = [swap(parts[r], r, n_sub) for r in range(n_sub)]
    return down(incoming, back, l2l_ops)


def solution(mesh):
    in_specs = (
        P(None, ("slab", "sub")),
        P(None, ("slab", "sub")),
        P(),
        P("sub", None, None),
        P(),
        P(None, ("slab", "sub")),
    )
    out_specs = P(None, ("slab", "sub"))
    return jax.shard_map(local, mesh=mesh, in_specs=in_specs, out_specs=out_specs, check_vma=False)
```

```python
import functools

import jax
import jax.numpy as jnp
from jax import lax
from jax.experimental import pallas as pl
from jax.experimental.pallas import tpu as pltpu
from jax.sharding import PartitionSpec as P

RIM = 32
TILE = 256
LANES = 128
GROUP = 4
VMEM = pl.BlockSpec(memory_space=pltpu.VMEM)
ANY = pl.BlockSpec(memory_space=pl.ANY)
BF16 = jnp.bfloat16
F32 = jnp.float32


def swap(x, r, n):
    return x if r == 0 else lax.ppermute(x, "sub", [(i, i ^ r) for i in range(n)])


def one_hot(mask):
    return jnp.where(mask, jnp.ones((), BF16), jnp.zeros((), BF16))


def half_rows(n_ops):
    return -(-n_ops // 16) * 16


def iota(shape, dim):
    return lax.broadcasted_iota(jnp.int32, shape, dim)


def up_kernel(n_sub, child_hbm, ops_hbm, partners_hbm, moments, codes, child, ops, partners, sems):
    copies = [
        pltpu.make_async_copy(src, dst, sems.at[i])
        for i, (src, dst) in enumerate([(child_hbm, child), (partners_hbm, partners), (ops_hbm, ops)])
    ]
    for copy in copies:
        copy.start()
    order, cells = moments.shape
    lane = iota((1, TILE), 1)
    row = iota((TILE, TILE), 0).astype(F32).astype(BF16)
    copies[0].wait()
    sorted_children = []
    for a in range(4):
        want = 8 * (lane % cells) + 2 * a + lane // cells
        cols = None
        for q in range(8 * cells // TILE):
            rel = (want - q * TILE).astype(F32).astype(BF16)
            hot = one_hot(row == jnp.broadcast_to(rel, (TILE, TILE)))
            part = jnp.dot(child[:, q * TILE : (q + 1) * TILE], hot, preferred_element_type=F32)
            cols = part if cols is None else cols + part
        sorted_children.append(cols.astype(BF16))

    copies[1].wait()
    n_ops = partners.shape[0] // n_sub
    my_slab = lax.axis_index("slab")
    codes[...] = jnp.zeros_like(codes)
    stride = half_rows(n_ops)
    for q in range(n_sub):
        ids = partners[q * n_ops : (q + 1) * n_ops, :]
        safe = jnp.maximum(ids, 0)
        source = lax.div(safe, cells)
        inner = safe - source * cells
        slab = lax.div(source, n_sub)
        block = (source - slab * n_sub) ^ q
        delta = slab - my_slab
        rim_at = n_sub * cells + block * (2 * RIM)
        column = jnp.where(
            delta == 0,
            block * cells + inner,
            jnp.where(delta < 0, rim_at + inner - (cells - RIM), rim_at + inner + RIM),
        )
        code = lax.shift_left(LANES + (column & (LANES - 1)), lax.shift_right_logical(column, 7))
        code = jnp.where(ids >= 0, code, 0).astype(F32)
        if stride > n_ops:
            code = jnp.concatenate([code, jnp.zeros((stride - n_ops, cells), F32)], axis=0)
        codes[q, 0:stride, :] = code[:, : cells // 2].astype(BF16)
        codes[q, stride : 2 * stride, :] = code[:, cells // 2 :].astype(BF16)

    copies[2].wait()
    total = None
    for a in range(4):
        for b in range(2):
            cols = sorted_children[a][:, b * cells : (b + 1) * cells]
            part = jnp.dot(ops[2 * a + b], cols, preferred_element_type=F32)
            total = part if total is None else total + part
    moments[...] = total.astype(BF16)


def up(child, ops, partners, n_sub):
    order = child.shape[0]
    cells = child.shape[1] // 8
    return pl.pallas_call(
        functools.partial(up_kernel, n_sub),
        out_shape=[
            jax.ShapeDtypeStruct((order, cells), BF16),
            jax.ShapeDtypeStruct((n_sub, order, cells // 2), BF16),
        ],
        in_specs=[ANY] * 3,
        out_specs=[VMEM] * 2,
        scratch_shapes=[
            pltpu.VMEM(child.shape, BF16),
            pltpu.VMEM(ops.shape, BF16),
            pltpu.VMEM(partners.shape, jnp.int32),
            pltpu.SemaphoreType.DMA((3,)),
        ],
        compiler_params=pltpu.CompilerParams(vmem_limit_bytes=50 << 20),
        cost_estimate=pl.CostEstimate(flops=1 << 30, bytes_accessed=2 << 20, transcendentals=0),
        name="up",
    )(child, ops, partners)


def fetch_kernel(after, src, dst, sems):
    chunk = src.shape[0] // sems.shape[0]
    copies = [
        pltpu.make_async_copy(src.at[pl.ds(i * chunk, chunk)], dst.at[pl.ds(i * chunk, chunk)], sems.at[i])
        for i in range(sems.shape[0])
    ]
    for copy in copies:
        copy.start()
    for copy in copies:
        copy.wait()


def fetch(after, x):
    return pl.pallas_call(
        fetch_kernel,
        out_shape=jax.ShapeDtypeStruct(x.shape, x.dtype),
        in_specs=[ANY, ANY],
        out_specs=VMEM,
        scratch_shapes=[pltpu.SemaphoreType.DMA((2,))],
        compiler_params=pltpu.CompilerParams(vmem_limit_bytes=8 << 20),
        cost_estimate=pl.CostEstimate(flops=1 << 30, bytes_accessed=4 << 20, transcendentals=0),
        name="fetch",
    )(after, x)


def m2l_kernel(n_sub, blocks, first, *refs):
    loads = refs[:n_sub]
    ops = refs[n_sub]
    rest = refs[n_sub + 1 :]
    if first:
        outs, (win, idx, code0, acc, cols, todo, scale) = rest[: len(blocks)], rest[len(blocks) :]
    else:
        win, outs, (idx, code0, acc, cols, todo, scale) = rest[0], rest[1 : len(blocks) + 1], rest[len(blocks) + 1 :]
    order, cells = outs[0].shape
    n_ops = ops.shape[0]
    n_tiles = acc.shape[0]
    k_tiles = win.shape[0]
    own_tiles = n_sub * cells // TILE
    stride = half_rows(n_ops)
    half = cells // 2

    if first:
        for r in range(n_sub):
            win[r * cells // TILE, :, r * cells % TILE : r * cells % TILE + cells] = loads[r][:, :cells]
        for b in range(n_sub // 2):
            pair = jnp.concatenate(
                [loads[2 * b][:, cells : cells + half], loads[2 * b + 1][:, cells : cells + half]], axis=1
            )
            at = b * cells
            win[own_tiles + at // TILE, :, at % TILE : at % TILE + cells] = pair
    rows = iota((TILE, LANES), 0)
    code0[...] = lax.shift_left(LANES + (rows & (LANES - 1)), lax.shift_right_logical(rows, 7)).astype(F32).astype(BF16)

    bits = lax.shift_left(1, iota((n_ops, 1), 0) & 31)
    words = {}
    for n in range(n_tiles):
        parts = []
        for r in blocks[n * TILE // cells : (n + 1) * TILE // cells]:
            parts.append(loads[r][0:stride, cells + half :].astype(F32)[:n_ops])
            parts.append(loads[r][stride : 2 * stride, cells + half :].astype(F32)[:n_ops])
        table = jnp.concatenate(parts, axis=1)
        idx[n, 0:n_ops, :] = table
        idx[n, n_ops : n_ops + 8, :] = jnp.zeros((8, TILE), F32)
        for t in range(k_tiles):
            low = float(LANES) * 4.0**t
            hit = jnp.where((table >= low) & (table < 4.0 * low), 1.0, 0.0)
            hit = jnp.max(hit, axis=1, keepdims=True)
            word = jnp.where(hit > 0.0, bits, 0)
            for w in range(-(-n_ops // 32)):
                words[n, t, w] = jnp.sum(word[32 * w : min(32 * w + 32, n_ops)])
    for t in range(k_tiles):
        scale[t] = jnp.float32(4.0**-t)

    count = jnp.int32(0)
    for (n, t, w), word in words.items():

        def more(state):
            return state[0] != 0

        def take(state, n=n, t=t, w=w):
            word, count = state
            k = 31 - lax.clz(word & -word)
            todo[count] = ((32 * w + k) * n_tiles + n) * k_tiles + t
            return word & (word - 1), count + 1

        count = lax.while_loop(more, take, (word, count))[1]
    for a in range(GROUP):
        todo[count + a] = n_ops * n_tiles * k_tiles
    trips = lax.div(count + GROUP - 1, GROUP)

    acc[...] = jnp.zeros_like(acc)
    cols[...] = jnp.zeros_like(cols)

    def unit(position):
        u = todo[position]
        kn = lax.div(u, k_tiles)
        k = lax.div(kn, n_tiles)
        return k, kn - k * n_tiles, u - kn * k_tiles

    def body(i, carry):
        slot = i & 1
        prev = 1 - slot
        base = code0[...]
        for a in range(GROUP):
            k, n, t = unit(jnp.minimum(GROUP * i + a, count))
            row = (idx[n, pl.ds(k, 1), :] * scale[t]).astype(BF16)
            hot = jnp.concatenate(
                [
                    one_hot(base == jnp.broadcast_to(row[:, c : c + LANES], (TILE, LANES)))
                    for c in range(0, TILE, LANES)
                ],
                axis=1,
            )
            cols[slot, a] = jnp.dot(win[t], hot, preferred_element_type=F32).astype(BF16)
        for a in range(GROUP):
            k, n, t = unit(jnp.clip(GROUP * (i - 1) + a, 0, count))
            acc[n] += jnp.dot(ops[jnp.minimum(k, n_ops - 1)], cols[prev, a], preferred_element_type=F32)
        return carry

    lax.fori_loop(0, trips + 1, body, 0)
    for j, out in enumerate(outs[: len(blocks)]):
        out[...] = acc[j * cells // TILE, :, j * cells % TILE : j * cells % TILE + cells].astype(out.dtype)


def m2l(loads, ops, cells, blocks, dtype, win=None):
    n_sub = len(loads)
    order = loads[0].shape[0]
    n_ops = ops.shape[0]
    n_tiles = len(blocks) * cells // TILE
    k_tiles = n_sub * (cells + 2 * RIM) // TILE
    units = n_ops * n_tiles * k_tiles
    out_shape = [jax.ShapeDtypeStruct((order, cells), dtype)] * len(blocks)
    args = [*loads, ops]
    if win is None:
        out_shape.append(jax.ShapeDtypeStruct((k_tiles, order, TILE), BF16))
    else:
        args.append(win)
    return pl.pallas_call(
        functools.partial(m2l_kernel, n_sub, blocks, win is None),
        out_shape=out_shape,
        in_specs=[VMEM] * len(args),
        out_specs=[VMEM] * len(out_shape),
        scratch_shapes=[
            pltpu.VMEM((n_tiles, n_ops + 8, TILE), F32),
            pltpu.VMEM((TILE, LANES), BF16),
            pltpu.VMEM((n_tiles, order, TILE), F32),
            pltpu.VMEM((2, GROUP, order, TILE), BF16),
            pltpu.SMEM((units + GROUP,), jnp.int32),
            pltpu.SMEM((k_tiles,), F32),
        ],
        compiler_params=pltpu.CompilerParams(vmem_limit_bytes=24 << 20),
        cost_estimate=pl.CostEstimate(flops=4 << 30, bytes_accessed=4 << 20, transcendentals=0),
        name="m2l",
    )(*args)


def down_kernel(n_parts, incoming, *refs):
    parts = refs[:n_parts]
    ops, out, stage, sem = refs[n_parts:]
    cells = incoming.shape[1]
    far = parts[0][...].astype(F32)
    for r in range(1, n_parts):
        far = far + parts[r][...].astype(F32)
    held = (incoming[...].astype(F32) + far).astype(BF16)
    lane = iota((1, TILE), 1)
    cell = iota((cells, TILE), 0).astype(F32).astype(BF16)
    octant = jnp.broadcast_to((lane % 8).astype(F32).astype(BF16), held.shape[:1] + (TILE,))
    copies = []
    for q in range(8 * cells // TILE):
        hot = one_hot(cell == jnp.broadcast_to((q * (TILE // 8) + lane // 8).astype(F32).astype(BF16), (cells, TILE)))
        spread = jnp.dot(held, hot, preferred_element_type=F32).astype(BF16)
        total = None
        for o in range(8):
            one = jnp.where(octant == jnp.full((), o, BF16), spread, jnp.zeros((), BF16))
            part = jnp.dot(ops[o], one, preferred_element_type=F32)
            total = part if total is None else total + part
        stage[q] = total
        copy = pltpu.make_async_copy(stage.at[q], out.at[:, q * TILE : (q + 1) * TILE], sem.at[q])
        copy.start()
        copies.append(copy)
    for copy in copies:
        copy.wait()


def down(incoming, parts, ops):
    order, cells = incoming.shape
    chunks = 8 * cells // TILE
    return pl.pallas_call(
        functools.partial(down_kernel, len(parts)),
        out_shape=jax.ShapeDtypeStruct((order, 8 * cells), F32),
        in_specs=[VMEM] * (len(parts) + 2),
        out_specs=pl.BlockSpec(memory_space=pl.ANY),
        scratch_shapes=[pltpu.VMEM((chunks, order, TILE), F32), pltpu.SemaphoreType.DMA((chunks,))],
        compiler_params=pltpu.CompilerParams(vmem_limit_bytes=16 << 20),
        cost_estimate=pl.CostEstimate(flops=1 << 30, bytes_accessed=2 << 20, transcendentals=0),
        name="down",
    )(incoming, *parts, ops)


def local(child_moments, incoming, m2m_ops, m2l_ops, l2l_ops, partners):
    cells = incoming.shape[1]
    n_sub = lax.axis_size("sub")
    n_slab = lax.axis_size("slab")
    assert n_sub & (n_sub - 1) == 0 and n_slab % 2 == 0
    me = lax.axis_index("sub")
    moments, codes = up(child_moments, m2m_ops, partners, n_sub)

    even = lax.axis_index("slab") % 2 == 0
    low, high = moments[:, :RIM], moments[:, cells - RIM :]
    pairs = [(i, i ^ 1) for i in range(n_slab)]
    other = [(i, ((i + 1) ^ 1) - 1) for i in range(1, n_slab - 1)]
    got_other = lax.ppermute(jnp.where(even, low, high), "slab", other)
    got_pair = lax.ppermute(jnp.where(even, high, low), "slab", pairs)
    held_ops = fetch(moments, m2l_ops)
    below = jnp.where(even, got_other, got_pair)
    above = jnp.where(even, got_pair, got_other)
    loads = []
    for r in range(n_sub):
        code = lax.dynamic_index_in_dim(codes, me ^ r, 0, keepdims=False)
        loads.append(swap(jnp.concatenate([moments, below, above, code], axis=1), r, n_sub))

    half = n_sub // 2
    *far, win = m2l(loads, held_ops, cells, tuple(range(half, n_sub)), BF16)
    got = swap(jnp.concatenate(far, axis=1), half, n_sub)
    near = m2l(loads, held_ops, cells, tuple(range(half)), F32, win)
    extra = [got[:, r * cells : (r + 1) * cells].astype(F32) for r in range(half)]
    while half > 1:
        half //= 2
        sent = [(near[r] + extra[r]).astype(BF16) for r in range(half, 2 * half)]
        got = swap(jnp.concatenate(sent, axis=1) if half > 1 else sent[0], half, n_sub)
        extra = [extra[r] + got[:, r * cells : (r + 1) * cells].astype(F32) for r in range(half)]
    return down(incoming, [near[0], extra[0]], l2l_ops)


def solution(mesh):
    in_specs = (
        P(None, ("slab", "sub")),
        P(None, ("slab", "sub")),
        P(),
        P("sub", None, None),
        P(),
        P(None, ("slab", "sub")),
    )
    out_specs = P(None, ("slab", "sub"))
    return jax.shard_map(local, mesh=mesh, in_specs=in_specs, out_specs=out_specs, check_vma=False)
```

```python
import functools

import jax
import jax.numpy as jnp
from jax import lax
from jax.experimental import pallas as pl
from jax.experimental.pallas import tpu as pltpu
from jax.sharding import PartitionSpec as P

RIM = 32
TILE = 256
LANES = 128
GROUP = 8
VMEM = pl.BlockSpec(memory_space=pltpu.VMEM)
ANY = pl.BlockSpec(memory_space=pl.ANY)
HBM = pl.BlockSpec(memory_space=pltpu.HBM)
BF16 = jnp.bfloat16
F32 = jnp.float32


def swap(x, r, n):
    return x if r == 0 else lax.ppermute(x, "sub", [(i, i ^ r) for i in range(n)])


def one_hot(mask):
    return jnp.where(mask, jnp.ones((), BF16), jnp.zeros((), BF16))


def half_rows(n_ops):
    return -(-n_ops // 16) * 16


def iota(shape, dim):
    return lax.broadcasted_iota(jnp.int32, shape, dim)


def up_kernel(n_sub, child_hbm, ops_hbm, partners_hbm, moments, codes, child, ops, partners, sems):
    copies = [
        pltpu.make_async_copy(src, dst, sems.at[i])
        for i, (src, dst) in enumerate([(child_hbm, child), (partners_hbm, partners), (ops_hbm, ops)])
    ]
    for copy in copies:
        copy.start()
    order, cells = moments.shape
    lane = iota((1, TILE), 1)
    row = iota((TILE, TILE), 0).astype(F32).astype(BF16)
    copies[0].wait()
    sorted_children = []
    for a in range(4):
        want = 8 * (lane % cells) + 2 * a + lane // cells
        cols = None
        for q in range(8 * cells // TILE):
            rel = (want - q * TILE).astype(F32).astype(BF16)
            hot = one_hot(row == jnp.broadcast_to(rel, (TILE, TILE)))
            part = jnp.dot(child[:, q * TILE : (q + 1) * TILE], hot, preferred_element_type=F32)
            cols = part if cols is None else cols + part
        sorted_children.append(cols.astype(BF16))

    copies[1].wait()
    n_ops = partners.shape[0] // n_sub
    my_slab = lax.axis_index("slab")
    codes[...] = jnp.zeros_like(codes)
    stride = half_rows(n_ops)
    for q in range(n_sub):
        ids = partners[q * n_ops : (q + 1) * n_ops, :]
        safe = jnp.maximum(ids, 0)
        source = lax.div(safe, cells)
        inner = safe - source * cells
        slab = lax.div(source, n_sub)
        block = (source - slab * n_sub) ^ q
        delta = slab - my_slab
        rim_at = n_sub * cells + block * (2 * RIM)
        column = jnp.where(
            delta == 0,
            block * cells + inner,
            jnp.where(delta < 0, rim_at + inner - (cells - RIM), rim_at + inner + RIM),
        )
        code = lax.shift_left(LANES + (column & (LANES - 1)), lax.shift_right_logical(column, 7))
        code = jnp.where(ids >= 0, code, 0).astype(F32)
        if stride > n_ops:
            code = jnp.concatenate([code, jnp.zeros((stride - n_ops, cells), F32)], axis=0)
        codes[q, 0:stride, :] = code[:, : cells // 2].astype(BF16)
        codes[q, stride : 2 * stride, :] = code[:, cells // 2 :].astype(BF16)

    copies[2].wait()
    total = None
    for a in range(4):
        for b in range(2):
            cols = sorted_children[a][:, b * cells : (b + 1) * cells]
            part = jnp.dot(ops[2 * a + b], cols, preferred_element_type=F32)
            total = part if total is None else total + part
    moments[...] = total.astype(BF16)


def up(child, ops, partners, n_sub):
    order = child.shape[0]
    cells = child.shape[1] // 8
    return pl.pallas_call(
        functools.partial(up_kernel, n_sub),
        out_shape=[
            jax.ShapeDtypeStruct((order, cells), BF16),
            jax.ShapeDtypeStruct((n_sub, order, cells // 2), BF16),
        ],
        in_specs=[HBM] * 3,
        out_specs=[VMEM] * 2,
        scratch_shapes=[
            pltpu.VMEM(child.shape, BF16),
            pltpu.VMEM(ops.shape, BF16),
            pltpu.VMEM(partners.shape, jnp.int32),
            pltpu.SemaphoreType.DMA((3,)),
        ],
        compiler_params=pltpu.CompilerParams(vmem_limit_bytes=50 << 20),
        cost_estimate=pl.CostEstimate(flops=1 << 30, bytes_accessed=2 << 20, transcendentals=0),
        name="up",
    )(*[pltpu.with_memory_space_constraint(x, pltpu.HBM) for x in (child, ops, partners)])


def fetch_kernel(after, src, dst, sems):
    chunk = src.shape[0] // sems.shape[0]
    copies = [
        pltpu.make_async_copy(src.at[pl.ds(i * chunk, chunk)], dst.at[pl.ds(i * chunk, chunk)], sems.at[i])
        for i in range(sems.shape[0])
    ]
    for copy in copies:
        copy.start()
    for copy in copies:
        copy.wait()


def fetch(after, x):
    return pl.pallas_call(
        fetch_kernel,
        out_shape=jax.ShapeDtypeStruct(x.shape, x.dtype),
        in_specs=[ANY, HBM],
        out_specs=VMEM,
        scratch_shapes=[pltpu.SemaphoreType.DMA((2,))],
        compiler_params=pltpu.CompilerParams(vmem_limit_bytes=8 << 20),
        cost_estimate=pl.CostEstimate(flops=1 << 30, bytes_accessed=4 << 20, transcendentals=0),
        name="fetch",
    )(after, pltpu.with_memory_space_constraint(x, pltpu.HBM))


def m2l_kernel(n_sub, blocks, first, *refs):
    loads = refs[:n_sub]
    ops = refs[n_sub]
    rest = refs[n_sub + 1 :]
    if first:
        outs, (win, idx, code0, acc, cols, todo, scale) = rest[: len(blocks)], rest[len(blocks) :]
    else:
        win, outs, (idx, code0, acc, cols, todo, scale) = rest[0], rest[1 : len(blocks) + 1], rest[len(blocks) + 1 :]
    order, cells = outs[0].shape
    n_ops = ops.shape[0]
    n_tiles = acc.shape[0]
    k_tiles = win.shape[0]
    own_tiles = n_sub * cells // TILE
    stride = half_rows(n_ops)
    half = cells // 2

    if first:
        for r in range(n_sub):
            win[r * cells // TILE, :, r * cells % TILE : r * cells % TILE + cells] = loads[r][:, :cells]
        for b in range(n_sub // 2):
            pair = jnp.concatenate(
                [loads[2 * b][:, cells : cells + half], loads[2 * b + 1][:, cells : cells + half]], axis=1
            )
            at = b * cells
            win[own_tiles + at // TILE, :, at % TILE : at % TILE + cells] = pair
    rows = iota((TILE, LANES), 0)
    code0[...] = lax.shift_left(LANES + (rows & (LANES - 1)), lax.shift_right_logical(rows, 7)).astype(F32).astype(BF16)

    bits = lax.shift_left(1, iota((n_ops, 1), 0) & 31)
    words = {}
    for n in range(n_tiles):
        parts = []
        for r in blocks[n * TILE // cells : (n + 1) * TILE // cells]:
            parts.append(loads[r][0:stride, cells + half :].astype(F32)[:n_ops])
            parts.append(loads[r][stride : 2 * stride, cells + half :].astype(F32)[:n_ops])
        table = jnp.concatenate(parts, axis=1)
        idx[n, 0:n_ops, :] = table
        idx[n, n_ops : n_ops + 8, :] = jnp.zeros((8, TILE), F32)
        for t in range(k_tiles):
            low = float(LANES) * 4.0**t
            hit = jnp.where((table >= low) & (table < 4.0 * low), 1.0, 0.0)
            hit = jnp.max(hit, axis=1, keepdims=True)
            word = jnp.where(hit > 0.0, bits, 0)
            for w in range(-(-n_ops // 32)):
                words[n, t, w] = jnp.sum(word[32 * w : min(32 * w + 32, n_ops)])
    for t in range(k_tiles):
        scale[t] = jnp.float32(4.0**-t)

    count = jnp.int32(0)
    for (n, t, w), word in words.items():

        def more(state):
            return state[0] != 0

        def take(state, n=n, t=t, w=w):
            word, count = state
            k = 31 - lax.clz(word & -word)
            todo[count] = ((32 * w + k) * n_tiles + n) * k_tiles + t
            return word & (word - 1), count + 1

        count = lax.while_loop(more, take, (word, count))[1]
    for a in range(GROUP):
        todo[count + a] = n_ops * n_tiles * k_tiles
    trips = lax.div(count + GROUP - 1, GROUP)

    acc[...] = jnp.zeros_like(acc)

    def unit(position):
        u = todo[position]
        kn = lax.div(u, k_tiles)
        k = lax.div(kn, n_tiles)
        return k, kn - k * n_tiles, u - kn * k_tiles

    def gather(i):
        base = code0[...]
        for a in range(GROUP):
            k, n, t = unit(jnp.minimum(GROUP * i + a, count))
            row = (idx[n, pl.ds(k, 1), :] * scale[t]).astype(BF16)
            hot = jnp.concatenate(
                [
                    one_hot(base == jnp.broadcast_to(row[:, c : c + LANES], (TILE, LANES)))
                    for c in range(0, TILE, LANES)
                ],
                axis=1,
            )
            cols[i & 1, a] = jnp.dot(win[t], hot, preferred_element_type=F32).astype(BF16)

    def apply(i):
        for a in range(GROUP):
            k, n, t = unit(jnp.minimum(GROUP * i + a, count))
            acc[n] += jnp.dot(ops[jnp.minimum(k, n_ops - 1)], cols[i & 1, a], preferred_element_type=F32)

    def body(i, carry):
        apply(i - 1)
        gather(i)
        return carry

    gather(0)
    lax.fori_loop(1, trips, body, 0)
    apply(jnp.maximum(trips - 1, 0))
    for j, out in enumerate(outs[: len(blocks)]):
        out[...] = acc[j * cells // TILE, :, j * cells % TILE : j * cells % TILE + cells].astype(out.dtype)


def m2l(loads, ops, cells, blocks, dtype, win=None):
    n_sub = len(loads)
    order = loads[0].shape[0]
    n_ops = ops.shape[0]
    n_tiles = len(blocks) * cells // TILE
    k_tiles = n_sub * (cells + 2 * RIM) // TILE
    units = n_ops * n_tiles * k_tiles
    out_shape = [jax.ShapeDtypeStruct((order, cells), dtype)] * len(blocks)
    args = [*loads, ops]
    if win is None:
        out_shape.append(jax.ShapeDtypeStruct((k_tiles, order, TILE), BF16))
    else:
        args.append(win)
    return pl.pallas_call(
        functools.partial(m2l_kernel, n_sub, blocks, win is None),
        out_shape=out_shape,
        in_specs=[VMEM] * len(args),
        out_specs=[VMEM] * len(out_shape),
        scratch_shapes=[
            pltpu.VMEM((n_tiles, n_ops + 8, TILE), F32),
            pltpu.VMEM((TILE, LANES), BF16),
            pltpu.VMEM((n_tiles, order, TILE), F32),
            pltpu.VMEM((2, GROUP, order, TILE), BF16),
            pltpu.SMEM((units + GROUP,), jnp.int32),
            pltpu.SMEM((k_tiles,), F32),
        ],
        compiler_params=pltpu.CompilerParams(vmem_limit_bytes=24 << 20),
        cost_estimate=pl.CostEstimate(flops=4 << 30, bytes_accessed=4 << 20, transcendentals=0),
        name="m2l",
    )(*args)


def down_kernel(n_parts, incoming, *refs):
    parts = refs[:n_parts]
    ops, out, stage, sem = refs[n_parts:]
    cells = incoming.shape[1]
    far = parts[0][...].astype(F32)
    for r in range(1, n_parts):
        far = far + parts[r][...].astype(F32)
    held = (incoming[...].astype(F32) + far).astype(BF16)
    lane = iota((1, TILE), 1)
    cell = iota((cells, TILE), 0).astype(F32).astype(BF16)
    octant = jnp.broadcast_to((lane % 8).astype(F32).astype(BF16), held.shape[:1] + (TILE,))
    copies = []
    for q in range(8 * cells // TILE):
        hot = one_hot(cell == jnp.broadcast_to((q * (TILE // 8) + lane // 8).astype(F32).astype(BF16), (cells, TILE)))
        spread = jnp.dot(held, hot, preferred_element_type=F32).astype(BF16)
        total = None
        for o in range(8):
            one = jnp.where(octant == jnp.full((), o, BF16), spread, jnp.zeros((), BF16))
            part = jnp.dot(ops[o], one, preferred_element_type=F32)
            total = part if total is None else total + part
        stage[q] = total
        copy = pltpu.make_async_copy(stage.at[q], out.at[:, q * TILE : (q + 1) * TILE], sem.at[q])
        copy.start()
        copies.append(copy)
    for copy in copies:
        copy.wait()


def down(incoming, parts, ops):
    order, cells = incoming.shape
    chunks = 8 * cells // TILE
    return pl.pallas_call(
        functools.partial(down_kernel, len(parts)),
        out_shape=jax.ShapeDtypeStruct((order, 8 * cells), F32),
        in_specs=[VMEM] * (len(parts) + 2),
        out_specs=pl.BlockSpec(memory_space=pl.ANY),
        scratch_shapes=[pltpu.VMEM((chunks, order, TILE), F32), pltpu.SemaphoreType.DMA((chunks,))],
        compiler_params=pltpu.CompilerParams(vmem_limit_bytes=16 << 20),
        cost_estimate=pl.CostEstimate(flops=1 << 30, bytes_accessed=2 << 20, transcendentals=0),
        name="down",
    )(incoming, *parts, ops)


def local(child_moments, incoming, m2m_ops, m2l_ops, l2l_ops, partners):
    cells = incoming.shape[1]
    n_sub = lax.axis_size("sub")
    n_slab = lax.axis_size("slab")
    assert n_sub & (n_sub - 1) == 0 and n_slab % 2 == 0
    me = lax.axis_index("sub")
    moments, codes = up(child_moments, m2m_ops, partners, n_sub)

    even = lax.axis_index("slab") % 2 == 0
    low, high = moments[:, :RIM], moments[:, cells - RIM :]
    pairs = [(i, i ^ 1) for i in range(n_slab)]
    other = [(i, ((i + 1) ^ 1) - 1) for i in range(1, n_slab - 1)]
    got_other = lax.ppermute(jnp.where(even, low, high), "slab", other)
    got_pair = lax.ppermute(jnp.where(even, high, low), "slab", pairs)
    held_ops = fetch(moments, m2l_ops)
    below = jnp.where(even, got_other, got_pair)
    above = jnp.where(even, got_pair, got_other)
    loads = []
    for r in range(n_sub):
        code = lax.dynamic_index_in_dim(codes, me ^ r, 0, keepdims=False)
        loads.append(swap(jnp.concatenate([moments, below, above, code], axis=1), r, n_sub))

    half = n_sub // 2
    *far, win = m2l(loads, held_ops, cells, tuple(range(half, n_sub)), BF16)
    got = swap(jnp.concatenate(far, axis=1), half, n_sub)
    near = m2l(loads, held_ops, cells, tuple(range(half)), F32, win)
    extra = [got[:, r * cells : (r + 1) * cells].astype(F32) for r in range(half)]
    while half > 1:
        half //= 2
        sent = [(near[r] + extra[r]).astype(BF16) for r in range(half, 2 * half)]
        got = swap(jnp.concatenate(sent, axis=1) if half > 1 else sent[0], half, n_sub)
        extra = [extra[r] + got[:, r * cells : (r + 1) * cells].astype(F32) for r in range(half)]
    return down(incoming, [near[0], extra[0]], l2l_ops)


def solution(mesh):
    in_specs = (
        P(None, ("slab", "sub")),
        P(None, ("slab", "sub")),
        P(),
        P("sub", None, None),
        P(),
        P(None, ("slab", "sub")),
    )
    out_specs = P(None, ("slab", "sub"))
    return jax.shard_map(local, mesh=mesh, in_specs=in_specs, out_specs=out_specs, check_vma=False)
```

```python
import functools

import jax
import jax.numpy as jnp
from jax import lax
from jax.experimental import pallas as pl
from jax.experimental.pallas import tpu as pltpu
from jax.sharding import PartitionSpec as P

RIM = 32
TILE = 256
LANES = 128
GROUP = 8
VMEM = pl.BlockSpec(memory_space=pltpu.VMEM)
ANY = pl.BlockSpec(memory_space=pl.ANY)
HBM = pl.BlockSpec(memory_space=pltpu.HBM)
BF16 = jnp.bfloat16
F32 = jnp.float32


def swap(x, r, n):
    return x if r == 0 else lax.ppermute(x, "sub", [(i, i ^ r) for i in range(n)])


def one_hot(mask):
    return jnp.where(mask, jnp.ones((), BF16), jnp.zeros((), BF16))


def iota(shape, dim):
    return lax.broadcasted_iota(jnp.int32, shape, dim)


def up_kernel(n_sub, cells, child_hbm, ops_hbm, partners_hbm, *refs):
    outs = refs[:n_sub]
    child, ops, partners, sems = refs[n_sub:]
    copies = [
        pltpu.make_async_copy(src, dst, sems.at[i])
        for i, (src, dst) in enumerate([(partners_hbm, partners), (child_hbm, child), (ops_hbm, ops)])
    ]
    for copy in copies:
        copy.start()
    order = child.shape[0]
    lane = iota((1, TILE), 1)
    row = iota((TILE, TILE), 0).astype(F32).astype(BF16)

    copies[0].wait()
    n_ops = partners.shape[0] // n_sub
    my_slab = lax.axis_index("slab")
    me = lax.axis_index("sub")
    for r in range(n_sub):
        q = me ^ r
        ids = partners[pl.ds(pl.multiple_of(q * n_ops, n_ops), n_ops), :]
        safe = jnp.maximum(ids, 0)
        source = lax.div(safe, cells)
        inner = safe - source * cells
        slab = lax.div(source, n_sub)
        block = (source - slab * n_sub) ^ q
        delta = slab - my_slab
        rim_at = n_sub * cells + block * RIM
        column = jnp.where(
            delta == 0,
            block * cells + inner,
            jnp.where(delta < 0, rim_at + inner - (cells - RIM), rim_at + n_sub * RIM + inner),
        )
        code = lax.shift_left(LANES + (column & (LANES - 1)), lax.shift_right_logical(column, 7))
        outs[r][order:, :] = jnp.where(ids >= 0, code, 0).astype(F32).astype(BF16)

    copies[1].wait()
    sorted_children = []
    for a in range(4):
        want = 8 * (lane % cells) + 2 * a + lane // cells
        cols = None
        for q in range(8 * cells // TILE):
            rel = (want - q * TILE).astype(F32).astype(BF16)
            hot = one_hot(row == jnp.broadcast_to(rel, (TILE, TILE)))
            part = jnp.dot(child[:, q * TILE : (q + 1) * TILE], hot, preferred_element_type=F32)
            cols = part if cols is None else cols + part
        sorted_children.append(cols.astype(BF16))
    copies[2].wait()
    total = None
    for a in range(4):
        for b in range(2):
            cols = sorted_children[a][:, b * cells : (b + 1) * cells]
            part = jnp.dot(ops[2 * a + b], cols, preferred_element_type=F32)
            total = part if total is None else total + part
    total = total.astype(BF16)
    for r in range(n_sub):
        outs[r][:order, :] = total


def up(child, ops, partners, n_sub):
    order = child.shape[0]
    cells = child.shape[1] // 8
    n_ops = partners.shape[0] // n_sub
    return pl.pallas_call(
        functools.partial(up_kernel, n_sub, cells),
        out_shape=[jax.ShapeDtypeStruct((order + n_ops, cells), BF16)] * n_sub,
        in_specs=[HBM] * 3,
        out_specs=[VMEM] * n_sub,
        scratch_shapes=[
            pltpu.VMEM(child.shape, BF16),
            pltpu.VMEM(ops.shape, BF16),
            pltpu.VMEM(partners.shape, jnp.int32),
            pltpu.SemaphoreType.DMA((3,)),
        ],
        compiler_params=pltpu.CompilerParams(vmem_limit_bytes=50 << 20),
        cost_estimate=pl.CostEstimate(flops=1 << 30, bytes_accessed=2 << 20, transcendentals=0),
        name="up",
    )(*[pltpu.with_memory_space_constraint(x, pltpu.HBM) for x in (child, ops, partners)])


def fetch_kernel(after, src, dst, sems):
    chunk = src.shape[0] // sems.shape[0]
    copies = [
        pltpu.make_async_copy(src.at[pl.ds(i * chunk, chunk)], dst.at[pl.ds(i * chunk, chunk)], sems.at[i])
        for i in range(sems.shape[0])
    ]
    for copy in copies:
        copy.start()
    for copy in copies:
        copy.wait()


def fetch(after, x):
    return pl.pallas_call(
        fetch_kernel,
        out_shape=jax.ShapeDtypeStruct(x.shape, x.dtype),
        in_specs=[ANY, HBM],
        out_specs=VMEM,
        scratch_shapes=[pltpu.SemaphoreType.DMA((2,))],
        compiler_params=pltpu.CompilerParams(vmem_limit_bytes=8 << 20),
        cost_estimate=pl.CostEstimate(flops=1 << 30, bytes_accessed=4 << 20, transcendentals=0),
        name="fetch",
    )(after, pltpu.with_memory_space_constraint(x, pltpu.HBM))


def m2l_kernel(order, blocks, first_tile, loads_n, sides_n, start_n, *refs):
    loads, refs = refs[:loads_n], refs[loads_n:]
    sides, refs = refs[:sides_n], refs[sides_n:]
    ops, refs = refs[0], refs[1:]
    start, refs = refs[:start_n], refs[start_n:]
    *outs, win, idx, code0, acc, cols, todo, scale = refs
    cells = loads[0].shape[1]
    n_ops = ops.shape[0]
    n_tiles = acc.shape[0]
    k_tiles = win.shape[0]

    at = 0
    for piece in sides if sides_n else loads:
        for c in range(0, piece.shape[1], LANES):
            win[at // TILE, :, at % TILE : at % TILE + LANES] = piece[:order, c : c + LANES]
            at += LANES
    rows = iota((TILE, LANES), 0)
    code0[...] = lax.shift_left(LANES + (rows & (LANES - 1)), lax.shift_right_logical(rows, 7)).astype(F32).astype(BF16)

    bits = lax.shift_left(1, iota((n_ops, 1), 0) & 31)
    words = {}
    for n in range(n_tiles):
        parts = [loads[r][order:, :].astype(F32) for r in blocks[n * TILE // cells : (n + 1) * TILE // cells]]
        table = jnp.concatenate(parts, axis=1)
        idx[n, 0:n_ops, :] = table
        idx[n, n_ops : n_ops + 8, :] = jnp.zeros((8, TILE), F32)
        for t in range(k_tiles):
            low = float(LANES) * 4.0 ** (first_tile + t)
            hit = jnp.where((table >= low) & (table < 4.0 * low), 1.0, 0.0)
            hit = jnp.max(hit, axis=1, keepdims=True)
            word = jnp.where(hit > 0.0, bits, 0)
            for w in range(-(-n_ops // 32)):
                words[n, t, w] = jnp.sum(word[32 * w : min(32 * w + 32, n_ops)])
    for t in range(k_tiles):
        scale[t] = jnp.float32(4.0 ** -(first_tile + t))

    count = jnp.int32(0)
    for (n, t, w), word in words.items():

        def more(state):
            return state[0] != 0

        def take(state, n=n, t=t, w=w):
            word, count = state
            k = 31 - lax.clz(word & -word)
            todo[count] = ((32 * w + k) * n_tiles + n) * k_tiles + t
            return word & (word - 1), count + 1

        count = lax.while_loop(more, take, (word, count))[1]
    for a in range(GROUP):
        todo[count + a] = n_ops * n_tiles * k_tiles
    trips = lax.div(count + GROUP - 1, GROUP)

    for n in range(n_tiles):
        acc[n] = start[n][...] if start_n else jnp.zeros_like(acc[n])

    def unit(position):
        u = todo[position]
        kn = lax.div(u, k_tiles)
        k = lax.div(kn, n_tiles)
        return k, kn - k * n_tiles, u - kn * k_tiles

    def gather(i):
        base = code0[...]
        for a in range(GROUP):
            k, n, t = unit(jnp.minimum(GROUP * i + a, count))
            row = (idx[n, pl.ds(k, 1), :] * scale[t]).astype(BF16)
            hot = jnp.concatenate(
                [
                    one_hot(base == jnp.broadcast_to(row[:, c : c + LANES], (TILE, LANES)))
                    for c in range(0, TILE, LANES)
                ],
                axis=1,
            )
            cols[i & 1, a] = jnp.dot(win[t], hot, preferred_element_type=F32).astype(BF16)

    def apply(i):
        for a in range(GROUP):
            k, n, t = unit(jnp.minimum(GROUP * i + a, count))
            acc[n] += jnp.dot(ops[jnp.minimum(k, n_ops - 1)], cols[i & 1, a], preferred_element_type=F32)

    def body(i, carry):
        apply(i - 1)
        gather(i)
        return carry

    gather(0)
    lax.fori_loop(1, trips, body, 0)
    apply(jnp.maximum(trips - 1, 0))
    wide = outs[0].shape[1]
    for j, out in enumerate(outs):
        out[...] = acc[j * wide // TILE, :, j * wide % TILE : j * wide % TILE + wide].astype(out.dtype)


def m2l(loads, ops, order, blocks, sides=(), start=(), dtype=None):
    n_sub = len(loads)
    cells = loads[0].shape[1]
    n_ops = ops.shape[0]
    n_tiles = len(blocks) * cells // TILE
    k_tiles = sum(x.shape[1] for x in (sides or loads)) // TILE
    units = n_ops * n_tiles * k_tiles
    args = [*loads, *sides, ops, *start]
    if dtype is None:
        out_shape = [jax.ShapeDtypeStruct((order, TILE), F32)] * n_tiles
    else:
        out_shape = [jax.ShapeDtypeStruct((order, cells), dtype)] * len(blocks)
    return pl.pallas_call(
        functools.partial(
            m2l_kernel, order, blocks, n_sub * cells // TILE if sides else 0, n_sub, len(sides), len(start)
        ),
        out_shape=out_shape,
        in_specs=[VMEM] * len(args),
        out_specs=[VMEM] * len(out_shape),
        scratch_shapes=[
            pltpu.VMEM((k_tiles, order, TILE), BF16),
            pltpu.VMEM((n_tiles, n_ops + 8, TILE), F32),
            pltpu.VMEM((TILE, LANES), BF16),
            pltpu.VMEM((n_tiles, order, TILE), F32),
            pltpu.VMEM((2, GROUP, order, TILE), BF16),
            pltpu.SMEM((units + GROUP,), jnp.int32),
            pltpu.SMEM((k_tiles,), F32),
        ],
        compiler_params=pltpu.CompilerParams(vmem_limit_bytes=24 << 20),
        cost_estimate=pl.CostEstimate(flops=4 << 30, bytes_accessed=4 << 20, transcendentals=0),
        name="m2l",
    )(*args)


def down_kernel(n_parts, incoming, *refs):
    parts = refs[:n_parts]
    ops, out, stage, sem = refs[n_parts:]
    cells = incoming.shape[1]
    far = parts[0][...].astype(F32)
    for r in range(1, n_parts):
        far = far + parts[r][...].astype(F32)
    held = (incoming[...].astype(F32) + far).astype(BF16)
    lane = iota((1, TILE), 1)
    cell = iota((cells, TILE), 0).astype(F32).astype(BF16)
    octant = jnp.broadcast_to((lane % 8).astype(F32).astype(BF16), held.shape[:1] + (TILE,))
    copies = []
    for q in range(8 * cells // TILE):
        hot = one_hot(cell == jnp.broadcast_to((q * (TILE // 8) + lane // 8).astype(F32).astype(BF16), (cells, TILE)))
        spread = jnp.dot(held, hot, preferred_element_type=F32).astype(BF16)
        total = None
        for o in range(8):
            one = jnp.where(octant == jnp.full((), o, BF16), spread, jnp.zeros((), BF16))
            part = jnp.dot(ops[o], one, preferred_element_type=F32)
            total = part if total is None else total + part
        stage[q] = total
        copy = pltpu.make_async_copy(stage.at[q], out.at[:, q * TILE : (q + 1) * TILE], sem.at[q])
        copy.start()
        copies.append(copy)
    for copy in copies:
        copy.wait()


def down(incoming, parts, ops):
    order, cells = incoming.shape
    chunks = 8 * cells // TILE
    return pl.pallas_call(
        functools.partial(down_kernel, len(parts)),
        out_shape=jax.ShapeDtypeStruct((order, 8 * cells), F32),
        in_specs=[VMEM] * (len(parts) + 2),
        out_specs=pl.BlockSpec(memory_space=pl.ANY),
        scratch_shapes=[pltpu.VMEM((chunks, order, TILE), F32), pltpu.SemaphoreType.DMA((chunks,))],
        compiler_params=pltpu.CompilerParams(vmem_limit_bytes=16 << 20),
        cost_estimate=pl.CostEstimate(flops=1 << 30, bytes_accessed=2 << 20, transcendentals=0),
        name="down",
    )(incoming, *parts, ops)


def local(child_moments, incoming, m2m_ops, m2l_ops, l2l_ops, partners):
    order, cells = incoming.shape
    n_sub = lax.axis_size("sub")
    n_slab = lax.axis_size("slab")
    assert n_sub & (n_sub - 1) == 0 and n_slab % 2 == 0
    sends = up(child_moments, m2m_ops, partners, n_sub)
    loads = [swap(sends[r], r, n_sub) for r in range(n_sub)]
    held_ops = fetch(sends[0], m2l_ops)

    even = lax.axis_index("slab") % 2 == 0
    low = jnp.concatenate([x[:order, :RIM] for x in loads], axis=1)
    high = jnp.concatenate([x[:order, cells - RIM :] for x in loads], axis=1)
    pairs = [(i, i ^ 1) for i in range(n_slab)]
    other = [(i, ((i + 1) ^ 1) - 1) for i in range(1, n_slab - 1)]
    got_other = lax.ppermute(jnp.where(even, low, high), "slab", other)
    got_pair = lax.ppermute(jnp.where(even, high, low), "slab", pairs)
    own = m2l(loads, held_ops, order, tuple(range(n_sub)))
    sides = [jnp.where(even, got_other, got_pair), jnp.where(even, got_pair, got_other)]

    half = n_sub // 2
    cut = half * cells // TILE
    far = m2l(loads, held_ops, order, tuple(range(half, n_sub)), sides, own[cut:], BF16)
    got = swap(jnp.concatenate(far, axis=1), half, n_sub)
    near = m2l(loads, held_ops, order, tuple(range(half)), sides, own[:cut], F32)
    extra = [got[:, r * cells : (r + 1) * cells].astype(F32) for r in range(half)]
    while half > 1:
        half //= 2
        sent = [(near[r] + extra[r]).astype(BF16) for r in range(half, 2 * half)]
        got = swap(jnp.concatenate(sent, axis=1) if half > 1 else sent[0], half, n_sub)
        extra = [extra[r] + got[:, r * cells : (r + 1) * cells].astype(F32) for r in range(half)]
    return down(incoming, [near[0], extra[0]], l2l_ops)


def solution(mesh):
    in_specs = (
        P(None, ("slab", "sub")),
        P(None, ("slab", "sub")),
        P(),
        P("sub", None, None),
        P(),
        P(None, ("slab", "sub")),
    )
    out_specs = P(None, ("slab", "sub"))
    return jax.shard_map(local, mesh=mesh, in_specs=in_specs, out_specs=out_specs, check_vma=False)
```

```python
import functools

import jax
import jax.numpy as jnp
from jax import lax
from jax.experimental import pallas as pl
from jax.experimental.pallas import tpu as pltpu
from jax.sharding import PartitionSpec as P

RIM = 32
TILE = 256
LANES = 128
GROUP = 8
VMEM = pl.BlockSpec(memory_space=pltpu.VMEM)
ANY = pl.BlockSpec(memory_space=pl.ANY)
HBM = pl.BlockSpec(memory_space=pltpu.HBM)
BF16 = jnp.bfloat16
F32 = jnp.float32


def swap(x, r, n):
    return x if r == 0 else lax.ppermute(x, "sub", [(i, i ^ r) for i in range(n)])


def one_hot(mask):
    return jnp.where(mask, jnp.ones((), BF16), jnp.zeros((), BF16))


def iota(shape, dim):
    return lax.broadcasted_iota(jnp.int32, shape, dim)


def up_kernel(n_sub, cells, child_hbm, ops_hbm, partners_hbm, *refs):
    outs, refs = refs[:n_sub], refs[n_sub:]
    to_pair, to_other, child, ops, partners, sems = refs
    copies = [
        pltpu.make_async_copy(src, dst, sems.at[i])
        for i, (src, dst) in enumerate([(partners_hbm, partners), (child_hbm, child), (ops_hbm, ops)])
    ]
    for copy in copies:
        copy.start()
    order = child.shape[0]
    lane = iota((1, TILE), 1)
    row = iota((TILE, TILE), 0).astype(F32).astype(BF16)

    copies[0].wait()
    n_ops = partners.shape[0] // n_sub
    my_slab = lax.axis_index("slab")
    me = lax.axis_index("sub")
    for r in range(n_sub):
        q = me ^ r
        ids = partners[pl.ds(pl.multiple_of(q * n_ops, n_ops), n_ops), :]
        safe = jnp.maximum(ids, 0)
        source = lax.div(safe, cells)
        inner = safe - source * cells
        slab = lax.div(source, n_sub)
        block = (source - slab * n_sub) ^ q
        delta = slab - my_slab
        rim_at = n_sub * cells + block * (2 * RIM)
        column = jnp.where(
            delta == 0,
            block * cells + inner,
            jnp.where(delta < 0, rim_at + inner - (cells - RIM), rim_at + RIM + inner),
        )
        code = lax.shift_left(LANES + (column & (LANES - 1)), lax.shift_right_logical(column, 7))
        outs[r][order:, :] = jnp.where(ids >= 0, code, 0).astype(F32).astype(BF16)

    copies[1].wait()
    sorted_children = []
    for a in range(4):
        want = 8 * (lane % cells) + 2 * a + lane // cells
        cols = None
        for q in range(8 * cells // TILE):
            rel = (want - q * TILE).astype(F32).astype(BF16)
            hot = one_hot(row == jnp.broadcast_to(rel, (TILE, TILE)))
            part = jnp.dot(child[:, q * TILE : (q + 1) * TILE], hot, preferred_element_type=F32)
            cols = part if cols is None else cols + part
        sorted_children.append(cols.astype(BF16))
    copies[2].wait()
    total = None
    for a in range(4):
        for b in range(2):
            cols = sorted_children[a][:, b * cells : (b + 1) * cells]
            part = jnp.dot(ops[2 * a + b], cols, preferred_element_type=F32)
            total = part if total is None else total + part
    total = total.astype(BF16)
    for r in range(n_sub):
        outs[r][:order, :] = total
    low, high = total[:, :RIM], total[:, cells - RIM :]
    even = lax.rem(my_slab, 2) == 0
    to_pair[...] = jnp.where(even, high, low)
    to_other[...] = jnp.where(even, low, high)


def up(child, ops, partners, n_sub):
    order = child.shape[0]
    cells = child.shape[1] // 8
    n_ops = partners.shape[0] // n_sub
    return pl.pallas_call(
        functools.partial(up_kernel, n_sub, cells),
        out_shape=[jax.ShapeDtypeStruct((order + n_ops, cells), BF16)] * n_sub
        + [jax.ShapeDtypeStruct((order, RIM), BF16)] * 2,
        in_specs=[HBM] * 3,
        out_specs=[VMEM] * (n_sub + 2),
        scratch_shapes=[
            pltpu.VMEM(child.shape, BF16),
            pltpu.VMEM(ops.shape, BF16),
            pltpu.VMEM(partners.shape, jnp.int32),
            pltpu.SemaphoreType.DMA((3,)),
        ],
        compiler_params=pltpu.CompilerParams(vmem_limit_bytes=16 << 20),
        cost_estimate=pl.CostEstimate(flops=1 << 30, bytes_accessed=2 << 20, transcendentals=0),
        name="up",
    )(*[pltpu.with_memory_space_constraint(x, pltpu.HBM) for x in (child, ops, partners)])


def m2l_kernel(order, blocks, first_tile, loads_n, sides_n, start_n, *refs):
    loads, refs = refs[:loads_n], refs[loads_n:]
    sides, refs = refs[:sides_n], refs[sides_n:]
    ops, refs = refs[0], refs[1:]
    start, refs = refs[:start_n], refs[start_n:]
    *outs, win, idx, code0, acc, cols, todo, scale, sems = refs
    fetching = not sides_n
    if fetching:
        ops_hbm, ops, outs = ops, outs[-1], outs[:-1]
    cells = loads[0].shape[1]
    n_ops = ops.shape[0]
    n_tiles = acc.shape[0]
    k_tiles = win.shape[0]

    at = 0
    if sides_n:
        pieces = [jnp.concatenate([sides[i][...], sides[i + 1][...]], axis=1) for i in range(0, sides_n, 2)]
    else:
        pieces = [x[:order, :] for x in loads]
    for piece in pieces:
        win[at // TILE, :, at % TILE : at % TILE + LANES] = piece
        at += LANES
    rows = iota((TILE, LANES), 0)
    code0[...] = lax.shift_left(LANES + (rows & (LANES - 1)), lax.shift_right_logical(rows, 7)).astype(F32).astype(BF16)

    bits = lax.shift_left(1, iota((n_ops, 1), 0) & 31)
    words = {}
    spans = [(w, min(32 * w + 32, n_ops)) for w in range(-(-n_ops // 32))]
    used = None

    def more(state):
        return state[0] != 0

    def lowest(word, w):
        return 32 * w + 31 - lax.clz(word & -word)

    def copy_in(k):
        return pltpu.make_async_copy(ops_hbm.at[k], ops.at[k], sems.at[k])

    def for_used(act):
        for w, word in enumerate(fetched):

            def one(state, w=w):
                act(copy_in(lowest(state[0], w)))
                return state[0] & (state[0] - 1), state[1]

            lax.while_loop(more, one, (word, jnp.int32(0)))

    for n in range(n_tiles):
        parts = [loads[r][order:, :].astype(F32) for r in blocks[n * TILE // cells : (n + 1) * TILE // cells]]
        table = jnp.concatenate(parts, axis=1)
        used = table if used is None else jnp.maximum(used, table)
        idx[n, 0:n_ops, :] = table
        idx[n, n_ops : n_ops + 8, :] = jnp.zeros((8, TILE), F32)
    if fetching:
        word = jnp.where(jnp.max(used, axis=1, keepdims=True) > 0.0, bits, 0)
        word = jnp.where(iota((n_ops, 1), 0) == n_ops - 1, bits, word)
        fetched = [jnp.sum(word[32 * w : end]) for w, end in spans]
        for_used(lambda copy: copy.start())
    for n in range(n_tiles):
        table = idx[n, 0:n_ops, :]
        for t in range(k_tiles):
            low = float(LANES) * 4.0 ** (first_tile + t)
            hit = jnp.where((table >= low) & (table < 4.0 * low), 1.0, 0.0)
            hit = jnp.max(hit, axis=1, keepdims=True)
            word = jnp.where(hit > 0.0, bits, 0)
            for w, end in spans:
                words[n, t, w] = jnp.sum(word[32 * w : end])
    for t in range(k_tiles):
        scale[t] = jnp.float32(4.0 ** -(first_tile + t))

    count = jnp.int32(0)
    for (n, t, w), word in words.items():

        def take(state, n=n, t=t, w=w):
            word, count = state
            todo[count] = (lowest(word, w) * n_tiles + n) * k_tiles + t
            return word & (word - 1), count + 1

        count = lax.while_loop(more, take, (word, count))[1]
    for a in range(GROUP):
        todo[count + a] = n_ops * n_tiles * k_tiles
    trips = lax.div(count + GROUP - 1, GROUP)

    for n in range(n_tiles):
        acc[n] = start[n][...] if start_n else jnp.zeros_like(acc[n])

    def unit(position):
        u = todo[position]
        kn = lax.div(u, k_tiles)
        k = lax.div(kn, n_tiles)
        return k, kn - k * n_tiles, u - kn * k_tiles

    def gather(i):
        base = code0[...]
        for a in range(GROUP):
            k, n, t = unit(jnp.minimum(GROUP * i + a, count))
            row = (idx[n, pl.ds(k, 1), :] * scale[t]).astype(BF16)
            hot = jnp.concatenate(
                [
                    one_hot(base == jnp.broadcast_to(row[:, c : c + LANES], (TILE, LANES)))
                    for c in range(0, TILE, LANES)
                ],
                axis=1,
            )
            cols[i & 1, a] = jnp.dot(win[t], hot, preferred_element_type=F32).astype(BF16)

    def apply(i):
        for a in range(GROUP):
            k, n, t = unit(jnp.minimum(GROUP * i + a, count))
            acc[n] += jnp.dot(ops[jnp.minimum(k, n_ops - 1)], cols[i & 1, a], preferred_element_type=F32)

    def body(i, carry):
        apply(i - 1)
        gather(i)
        return carry

    gather(0)
    if fetching:
        for_used(lambda copy: copy.wait())
    lax.fori_loop(1, trips, body, 0)
    apply(jnp.maximum(trips - 1, 0))
    wide = outs[0].shape[1]
    for j, out in enumerate(outs):
        out[...] = acc[j * wide // TILE, :, j * wide % TILE : j * wide % TILE + wide].astype(out.dtype)


def m2l(loads, ops, order, blocks, sides=(), start=(), dtype=None):
    n_sub = len(loads)
    cells = loads[0].shape[1]
    n_ops = ops.shape[0]
    n_tiles = len(blocks) * cells // TILE
    k_tiles = sum(x.shape[1] for x in (sides or loads)) // TILE
    units = n_ops * n_tiles * k_tiles
    args = [*loads, *sides, ops, *start]
    specs = [VMEM] * len(args)
    if dtype is None:
        out_shape = [jax.ShapeDtypeStruct((order, TILE), F32)] * n_tiles + [jax.ShapeDtypeStruct(ops.shape, BF16)]
        args[n_sub] = pltpu.with_memory_space_constraint(ops, pltpu.HBM)
        specs[n_sub] = HBM
    else:
        out_shape = [jax.ShapeDtypeStruct((order, cells), F32 if r == 0 else dtype) for r in blocks]
    return pl.pallas_call(
        functools.partial(
            m2l_kernel, order, blocks, n_sub * cells // TILE if sides else 0, n_sub, len(sides), len(start)
        ),
        out_shape=out_shape,
        in_specs=specs,
        out_specs=[VMEM] * len(out_shape),
        scratch_shapes=[
            pltpu.VMEM((k_tiles, order, TILE), BF16),
            pltpu.VMEM((n_tiles, n_ops + 8, TILE), F32),
            pltpu.VMEM((TILE, LANES), BF16),
            pltpu.VMEM((n_tiles, order, TILE), F32),
            pltpu.VMEM((2, GROUP, order, TILE), BF16),
            pltpu.SMEM((units + GROUP,), jnp.int32),
            pltpu.SMEM((k_tiles,), F32),
            pltpu.SemaphoreType.DMA((n_ops,)),
        ],
        compiler_params=pltpu.CompilerParams(vmem_limit_bytes=16 << 20),
        cost_estimate=pl.CostEstimate(flops=4 << 30, bytes_accessed=4 << 20, transcendentals=0),
        name="m2l",
    )(*args)


def down_kernel(n_parts, incoming, *refs):
    parts = refs[:n_parts]
    ops, out, stage, sem = refs[n_parts:]
    cells = incoming.shape[1]
    far = parts[0][...].astype(F32)
    for r in range(1, n_parts):
        far = far + parts[r][...].astype(F32)
    held = (incoming[...].astype(F32) + far).astype(BF16)
    lane = iota((1, TILE), 1)
    cell = iota((cells, TILE), 0).astype(F32).astype(BF16)
    octant = jnp.broadcast_to((lane % 8).astype(F32).astype(BF16), held.shape[:1] + (TILE,))
    copies = []
    for q in range(8 * cells // TILE):
        hot = one_hot(cell == jnp.broadcast_to((q * (TILE // 8) + lane // 8).astype(F32).astype(BF16), (cells, TILE)))
        spread = jnp.dot(held, hot, preferred_element_type=F32).astype(BF16)
        total = None
        for o in range(8):
            one = jnp.where(octant == jnp.full((), o, BF16), spread, jnp.zeros((), BF16))
            part = jnp.dot(ops[o], one, preferred_element_type=F32)
            total = part if total is None else total + part
        stage[q] = total
        copy = pltpu.make_async_copy(stage.at[q], out.at[:, q * TILE : (q + 1) * TILE], sem.at[q])
        copy.start()
        copies.append(copy)
    for copy in copies:
        copy.wait()


def down(incoming, parts, ops):
    order, cells = incoming.shape
    chunks = 8 * cells // TILE
    return pl.pallas_call(
        functools.partial(down_kernel, len(parts)),
        out_shape=jax.ShapeDtypeStruct((order, 8 * cells), F32),
        in_specs=[VMEM] * (len(parts) + 2),
        out_specs=pl.BlockSpec(memory_space=pl.ANY),
        scratch_shapes=[pltpu.VMEM((chunks, order, TILE), F32), pltpu.SemaphoreType.DMA((chunks,))],
        compiler_params=pltpu.CompilerParams(vmem_limit_bytes=16 << 20),
        cost_estimate=pl.CostEstimate(flops=1 << 30, bytes_accessed=2 << 20, transcendentals=0),
        name="down",
    )(incoming, *parts, ops)


def local(child_moments, incoming, m2m_ops, m2l_ops, l2l_ops, partners):
    order, cells = incoming.shape
    n_sub = lax.axis_size("sub")
    n_slab = lax.axis_size("slab")
    assert n_sub & (n_sub - 1) == 0 and n_slab % 2 == 0 and cells == LANES == 4 * RIM
    *sends, to_pair, to_other = up(child_moments, m2m_ops, partners, n_sub)
    got_other = lax.ppermute(to_other, "slab", [(i, ((i + 1) ^ 1) - 1) for i in range(1, n_slab - 1)])
    got_pair = lax.ppermute(to_pair, "slab", [(i, i ^ 1) for i in range(n_slab)])
    loads = [swap(sends[r], r, n_sub) for r in range(n_sub)]
    even = lax.axis_index("slab") % 2 == 0
    rim = jnp.concatenate(
        [jnp.where(even, got_other, got_pair), jnp.where(even, got_pair, got_other)], axis=1
    )
    sides = [swap(rim, r, n_sub) for r in range(n_sub)]
    blocks = tuple(range(n_sub))
    *own, held_ops = m2l(loads, m2l_ops, order, blocks)
    mine, *others = m2l(loads, held_ops, order, blocks, sides, own, BF16)
    back = [swap(x, r + 1, n_sub) for r, x in reversed(list(enumerate(others)))]
    return down(incoming, [mine, *back], l2l_ops)


def solution(mesh):
    in_specs = (
        P(None, ("slab", "sub")),
        P(None, ("slab", "sub")),
        P(),
        P("sub", None, None),
        P(),
        P(None, ("slab", "sub")),
    )
    out_specs = P(None, ("slab", "sub"))
    return jax.shard_map(local, mesh=mesh, in_specs=in_specs, out_specs=out_specs, check_vma=False)
```

```python
import functools

import jax
import jax.numpy as jnp
from jax import lax
from jax.experimental import pallas as pl
from jax.experimental.pallas import tpu as pltpu
from jax.sharding import PartitionSpec as P

RIM = 32
TILE = 256
LANES = 128
GROUP = 8
VMEM = pl.BlockSpec(memory_space=pltpu.VMEM)
ANY = pl.BlockSpec(memory_space=pl.ANY)
HBM = pl.BlockSpec(memory_space=pltpu.HBM)
BF16 = jnp.bfloat16
F32 = jnp.float32


def swap(x, r, n):
    return x if r == 0 else lax.ppermute(x, "sub", [(i, i ^ r) for i in range(n)])


def one_hot(mask):
    return jnp.where(mask, jnp.ones((), BF16), jnp.zeros((), BF16))


def iota(shape, dim):
    return lax.broadcasted_iota(jnp.int32, shape, dim)


def up_kernel(n_sub, cells, child_hbm, ops_hbm, partners_hbm, *refs):
    outs, refs = refs[:n_sub], refs[n_sub:]
    to_pair, to_other, child, ops, partners, sems = refs
    copies = [
        pltpu.make_async_copy(src, dst, sems.at[i])
        for i, (src, dst) in enumerate([(partners_hbm, partners), (child_hbm, child), (ops_hbm, ops)])
    ]
    for copy in copies:
        copy.start()
    order = child.shape[0]
    lane = iota((1, TILE), 1)
    row = iota((TILE, TILE), 0).astype(F32).astype(BF16)

    copies[0].wait()
    n_ops = partners.shape[0] // n_sub
    my_slab = lax.axis_index("slab")
    me = lax.axis_index("sub")
    for r in range(n_sub):
        q = me ^ r
        ids = partners[pl.ds(pl.multiple_of(q * n_ops, n_ops), n_ops), :]
        safe = jnp.maximum(ids, 0)
        source = lax.div(safe, cells)
        inner = safe - source * cells
        slab = lax.div(source, n_sub)
        block = (source - slab * n_sub) ^ q
        delta = slab - my_slab
        rim_at = n_sub * cells + block * (2 * RIM)
        column = jnp.where(
            delta == 0,
            block * cells + inner,
            jnp.where(delta < 0, rim_at + inner - (cells - RIM), rim_at + RIM + inner),
        )
        code = lax.shift_left(LANES + (column & (LANES - 1)), lax.shift_right_logical(column, 7))
        outs[r][order:, :] = jnp.where(ids >= 0, code, 0).astype(F32).astype(BF16)

    copies[1].wait()
    sorted_children = []
    for a in range(4):
        want = 8 * (lane % cells) + 2 * a + lane // cells
        cols = None
        for q in range(8 * cells // TILE):
            rel = (want - q * TILE).astype(F32).astype(BF16)
            hot = one_hot(row == jnp.broadcast_to(rel, (TILE, TILE)))
            part = jnp.dot(child[:, q * TILE : (q + 1) * TILE], hot, preferred_element_type=F32)
            cols = part if cols is None else cols + part
        sorted_children.append(cols.astype(BF16))
    copies[2].wait()
    total = None
    for a in range(4):
        for b in range(2):
            cols = sorted_children[a][:, b * cells : (b + 1) * cells]
            part = jnp.dot(ops[2 * a + b], cols, preferred_element_type=F32)
            total = part if total is None else total + part
    total = total.astype(BF16)
    for r in range(n_sub):
        outs[r][:order, :] = total
    low, high = total[:, :RIM], total[:, cells - RIM :]
    even = lax.rem(my_slab, 2) == 0
    to_pair[...] = jnp.where(even, high, low)
    to_other[...] = jnp.where(even, low, high)


def up(child, ops, partners, n_sub):
    order = child.shape[0]
    cells = child.shape[1] // 8
    n_ops = partners.shape[0] // n_sub
    return pl.pallas_call(
        functools.partial(up_kernel, n_sub, cells),
        out_shape=[jax.ShapeDtypeStruct((order + n_ops, cells), BF16)] * n_sub
        + [jax.ShapeDtypeStruct((order, RIM), BF16)] * 2,
        in_specs=[HBM] * 3,
        out_specs=[VMEM] * (n_sub + 2),
        scratch_shapes=[
            pltpu.VMEM(child.shape, BF16),
            pltpu.VMEM(ops.shape, BF16),
            pltpu.VMEM(partners.shape, jnp.int32),
            pltpu.SemaphoreType.DMA((3,)),
        ],
        compiler_params=pltpu.CompilerParams(vmem_limit_bytes=16 << 20),
        cost_estimate=pl.CostEstimate(flops=1 << 30, bytes_accessed=2 << 20, transcendentals=0),
        name="up",
    )(*[pltpu.with_memory_space_constraint(x, pltpu.HBM) for x in (child, ops, partners)])


def spans_of(n_ops):
    return [(w, min(w + 32, n_ops)) for w in range(0, n_ops, 32)]


def pack(hit, n_ops):
    word = jnp.where(hit > 0.0, lax.shift_left(1, iota((n_ops, 1), 0) & 31), 0)
    return [jnp.sum(word[w:end]) for w, end in spans_of(n_ops)]


def each_bit(words, act, state):
    for i, word in enumerate(words):

        def step(carry, i=i):
            word, state = carry
            return word & (word - 1), act(32 * i + 31 - lax.clz(word & -word), state)

        state = lax.while_loop(lambda carry: carry[0] != 0, step, (word, state))[1]
    return state


def list_units(order, loads, n_ops, idx, code0, todo):
    cells = loads[0].shape[1]
    n_tiles = idx.shape[0]
    per = TILE // cells
    rows = iota((TILE, LANES), 0)
    code0[...] = lax.shift_left(LANES + (rows & (LANES - 1)), lax.shift_right_logical(rows, 7)).astype(F32).astype(BF16)
    hits = []
    for n in range(n_tiles):
        table = jnp.concatenate([x[order:, :].astype(F32) for x in loads[n * per : (n + 1) * per]], axis=1)
        idx[n, 0:n_ops, :] = table
        idx[n, n_ops : n_ops + 8, :] = jnp.zeros((8, TILE), F32)
        hits.append(jnp.max(table, axis=1, keepdims=True))
    count = jnp.int32(0)
    for n in range(n_tiles):

        def add(k, count, n=n):
            todo[count] = k * n_tiles + n
            return count + 1

        count = each_bit(pack(hits[n], n_ops), add, count)
    for a in range(GROUP):
        todo[count + a] = n_ops * n_tiles
    return hits, count, lax.div(count + GROUP - 1, GROUP)


def one_hots(row, base, first_tile, n_tiles):
    for t in range(first_tile, first_tile + n_tiles):
        scaled = (row * (4.0**-t)).astype(BF16)
        yield jnp.concatenate(
            [
                one_hot(base == jnp.broadcast_to(scaled[:, c : c + LANES], (TILE, LANES)))
                for c in range(0, TILE, LANES)
            ],
            axis=1,
        )


def pick_kernel(order, n_sub, *refs):
    loads, refs = refs[:n_sub], refs[n_sub:]
    ops_hbm, picked, ops, win, idx, code0, todo, sems = refs
    n_ops = ops.shape[0]
    n_tiles, k_tiles = idx.shape[0], win.shape[0]
    cells = loads[0].shape[1]
    for r in range(n_sub):
        win[r * cells // TILE, :, r * cells % TILE : r * cells % TILE + cells] = loads[r][:order, :]
    hits, count, trips = list_units(order, loads, n_ops, idx, code0, todo)

    used = jnp.where(iota((n_ops, 1), 0) == n_ops - 1, 1.0, functools.reduce(jnp.maximum, hits))
    used = pack(used, n_ops)

    def copy_in(k):
        return pltpu.make_async_copy(ops_hbm.at[k], ops.at[k], sems.at[k])

    def start(k, state):
        copy_in(k).start()
        return state

    def wait(k, state):
        copy_in(k).wait()
        return state

    each_bit(used, start, jnp.int32(0))

    def body(i, carry):
        base = code0[...]
        for a in range(GROUP):
            u = todo[GROUP * i + a]
            k = lax.div(u, n_tiles)
            row = idx[u - k * n_tiles, pl.ds(k, 1), :]
            total = None
            for t, hot in enumerate(one_hots(row, base, 0, k_tiles)):
                part = jnp.dot(win[t], hot, preferred_element_type=F32)
                total = part if total is None else total + part
            picked[GROUP * i + a] = total.astype(BF16)
        return carry

    lax.fori_loop(0, trips, body, 0)
    each_bit(used, wait, jnp.int32(0))


def apply_kernel(order, n_sub, *refs):
    loads, sides, refs = refs[:n_sub], refs[n_sub : 2 * n_sub], refs[2 * n_sub :]
    picked, ops, refs = refs[0], refs[1], refs[2:]
    outs, (win, idx, code0, acc, cols, todo) = refs[:n_sub], refs[n_sub:]
    n_ops = ops.shape[0]
    n_tiles, k_tiles = idx.shape[0], win.shape[0]
    cells = loads[0].shape[1]
    for i in range(0, n_sub, 2):
        at = i // 2 * LANES
        pair = jnp.concatenate([sides[i][...], sides[i + 1][...]], axis=1)
        win[at // TILE, :, at % TILE : at % TILE + LANES] = pair
    _, count, trips = list_units(order, loads, n_ops, idx, code0, todo)
    acc[...] = jnp.zeros_like(acc)

    def gather(i):
        base = code0[...]
        for a in range(GROUP):
            u = todo[GROUP * i + a]
            k = lax.div(u, n_tiles)
            row = idx[u - k * n_tiles, pl.ds(k, 1), :]
            total = None
            for t, hot in enumerate(one_hots(row, base, n_sub * cells // TILE, k_tiles)):
                part = jnp.dot(win[t], hot, preferred_element_type=F32)
                total = part if total is None else total + part
            cols[i & 1, a] = total.astype(BF16) + picked[GROUP * i + a]

    def apply(i):
        for a in range(GROUP):
            u = todo[GROUP * i + a]
            k = lax.div(u, n_tiles)
            acc[u - k * n_tiles] += jnp.dot(
                ops[jnp.minimum(k, n_ops - 1)], cols[i & 1, a], preferred_element_type=F32
            )

    def body(i, carry):
        apply(i - 1)
        gather(i)
        return carry

    @pl.when(trips > 0)
    def _():
        gather(0)
        lax.fori_loop(1, trips, body, 0)
        apply(trips - 1)

    for j, out in enumerate(outs):
        out[...] = acc[j * cells // TILE, :, j * cells % TILE : j * cells % TILE + cells].astype(out.dtype)


def m2l_sizes(loads, ops):
    n_sub, cells = len(loads), loads[0].shape[1]
    n_tiles = n_sub * cells // TILE
    return n_sub, cells, n_tiles, ops.shape[0] * n_tiles + GROUP


def pick(loads, ops, order):
    n_sub, cells, n_tiles, units = m2l_sizes(loads, ops)
    n_ops = ops.shape[0]
    return pl.pallas_call(
        functools.partial(pick_kernel, order, n_sub),
        out_shape=[jax.ShapeDtypeStruct((units, order, TILE), BF16), jax.ShapeDtypeStruct(ops.shape, BF16)],
        in_specs=[VMEM] * n_sub + [HBM],
        out_specs=[VMEM] * 2,
        scratch_shapes=[
            pltpu.VMEM((n_sub * cells // TILE, order, TILE), BF16),
            pltpu.VMEM((n_tiles, n_ops + 8, TILE), F32),
            pltpu.VMEM((TILE, LANES), BF16),
            pltpu.SMEM((units,), jnp.int32),
            pltpu.SemaphoreType.DMA((n_ops,)),
        ],
        compiler_params=pltpu.CompilerParams(vmem_limit_bytes=24 << 20),
        cost_estimate=pl.CostEstimate(flops=4 << 30, bytes_accessed=4 << 20, transcendentals=0),
        name="pick",
    )(*loads, pltpu.with_memory_space_constraint(ops, pltpu.HBM))


def apply_ops(loads, sides, picked, ops, order):
    n_sub, cells, n_tiles, units = m2l_sizes(loads, ops)
    n_ops = ops.shape[0]
    return pl.pallas_call(
        functools.partial(apply_kernel, order, n_sub),
        out_shape=[jax.ShapeDtypeStruct((order, cells), F32 if r == 0 else BF16) for r in range(n_sub)],
        in_specs=[VMEM] * (2 * n_sub + 2),
        out_specs=[VMEM] * n_sub,
        scratch_shapes=[
            pltpu.VMEM((n_sub * 2 * RIM // TILE, order, TILE), BF16),
            pltpu.VMEM((n_tiles, n_ops + 8, TILE), F32),
            pltpu.VMEM((TILE, LANES), BF16),
            pltpu.VMEM((n_tiles, order, TILE), F32),
            pltpu.VMEM((2, GROUP, order, TILE), BF16),
            pltpu.SMEM((units,), jnp.int32),
        ],
        compiler_params=pltpu.CompilerParams(vmem_limit_bytes=24 << 20),
        cost_estimate=pl.CostEstimate(flops=4 << 30, bytes_accessed=4 << 20, transcendentals=0),
        name="apply",
    )(*loads, *sides, picked, ops)


def down_kernel(n_parts, incoming, *refs):
    parts = refs[:n_parts]
    ops, out, stage, sem = refs[n_parts:]
    cells = incoming.shape[1]
    far = parts[0][...].astype(F32)
    for r in range(1, n_parts):
        far = far + parts[r][...].astype(F32)
    held = (incoming[...].astype(F32) + far).astype(BF16)
    lane = iota((1, TILE), 1)
    cell = iota((cells, TILE), 0).astype(F32).astype(BF16)
    octant = jnp.broadcast_to((lane % 8).astype(F32).astype(BF16), held.shape[:1] + (TILE,))
    copies = []
    for q in range(8 * cells // TILE):
        hot = one_hot(cell == jnp.broadcast_to((q * (TILE // 8) + lane // 8).astype(F32).astype(BF16), (cells, TILE)))
        spread = jnp.dot(held, hot, preferred_element_type=F32).astype(BF16)
        total = None
        for o in range(8):
            one = jnp.where(octant == jnp.full((), o, BF16), spread, jnp.zeros((), BF16))
            part = jnp.dot(ops[o], one, preferred_element_type=F32)
            total = part if total is None else total + part
        stage[q] = total
        copy = pltpu.make_async_copy(stage.at[q], out.at[:, q * TILE : (q + 1) * TILE], sem.at[q])
        copy.start()
        copies.append(copy)
    for copy in copies:
        copy.wait()


def down(incoming, parts, ops):
    order, cells = incoming.shape
    chunks = 8 * cells // TILE
    return pl.pallas_call(
        functools.partial(down_kernel, len(parts)),
        out_shape=jax.ShapeDtypeStruct((order, 8 * cells), F32),
        in_specs=[VMEM] * (len(parts) + 2),
        out_specs=pl.BlockSpec(memory_space=pl.ANY),
        scratch_shapes=[pltpu.VMEM((chunks, order, TILE), F32), pltpu.SemaphoreType.DMA((chunks,))],
        compiler_params=pltpu.CompilerParams(vmem_limit_bytes=16 << 20),
        cost_estimate=pl.CostEstimate(flops=1 << 30, bytes_accessed=2 << 20, transcendentals=0),
        name="down",
    )(incoming, *parts, ops)


def local(child_moments, incoming, m2m_ops, m2l_ops, l2l_ops, partners):
    order, cells = incoming.shape
    n_sub = lax.axis_size("sub")
    n_slab = lax.axis_size("slab")
    assert n_sub & (n_sub - 1) == 0 and n_slab % 2 == 0 and cells == LANES == 4 * RIM
    *sends, to_pair, to_other = up(child_moments, m2m_ops, partners, n_sub)
    got_other = lax.ppermute(to_other, "slab", [(i, ((i + 1) ^ 1) - 1) for i in range(1, n_slab - 1)])
    got_pair = lax.ppermute(to_pair, "slab", [(i, i ^ 1) for i in range(n_slab)])
    loads = [swap(sends[r], r, n_sub) for r in range(n_sub)]
    even = lax.axis_index("slab") % 2 == 0
    rim = jnp.concatenate(
        [jnp.where(even, got_other, got_pair), jnp.where(even, got_pair, got_other)], axis=1
    )
    sides = [swap(rim, r, n_sub) for r in range(n_sub)]
    picked, held_ops = pick(loads, m2l_ops, order)
    mine, *others = apply_ops(loads, sides, picked, held_ops, order)
    back = [swap(x, r + 1, n_sub) for r, x in reversed(list(enumerate(others)))]
    return down(incoming, [mine, *back], l2l_ops)


def solution(mesh):
    in_specs = (
        P(None, ("slab", "sub")),
        P(None, ("slab", "sub")),
        P(),
        P("sub", None, None),
        P(),
        P(None, ("slab", "sub")),
    )
    out_specs = P(None, ("slab", "sub"))
    return jax.shard_map(local, mesh=mesh, in_specs=in_specs, out_specs=out_specs, check_vma=False)
```

```python
import functools

import jax
import jax.numpy as jnp
from jax import lax
from jax.experimental import pallas as pl
from jax.experimental.pallas import tpu as pltpu
from jax.sharding import PartitionSpec as P

RIM = 32
TILE = 256
LANES = 128
GROUP = 8
VMEM = pl.BlockSpec(memory_space=pltpu.VMEM)
ANY = pl.BlockSpec(memory_space=pl.ANY)
HBM = pl.BlockSpec(memory_space=pltpu.HBM)
BF16 = jnp.bfloat16
F32 = jnp.float32


def swap(x, r, n):
    return x if r == 0 else lax.ppermute(x, "sub", [(i, i ^ r) for i in range(n)])


def one_hot(mask):
    return jnp.where(mask, jnp.ones((), BF16), jnp.zeros((), BF16))


def by_group(groups, parts, shift):
    out = parts[shift % 4]
    for g in range(1, 4):
        out = jnp.where(groups == jnp.full((), g, groups.dtype), parts[(g + shift) % 4], out)
    return out


def iota(shape, dim):
    return lax.broadcasted_iota(jnp.int32, shape, dim)


def up_kernel(n_sub, cells, child_hbm, ops_hbm, partners_hbm, *refs):
    outs, refs = refs[:n_sub], refs[n_sub:]
    to_pair, to_other, child, ops, partners, sems = refs
    copies = [
        pltpu.make_async_copy(src, dst, sems.at[i])
        for i, (src, dst) in enumerate([(partners_hbm, partners), (child_hbm, child), (ops_hbm, ops)])
    ]
    for copy in copies:
        copy.start()
    order = child.shape[0]
    lane = iota((1, TILE), 1)
    row = iota((TILE, TILE), 0).astype(F32).astype(BF16)

    copies[0].wait()
    n_ops = partners.shape[0] // n_sub
    my_slab = lax.axis_index("slab")
    me = lax.axis_index("sub")
    for r in range(n_sub):
        q = me ^ r
        ids = partners[pl.ds(pl.multiple_of(q * n_ops, n_ops), n_ops), :]
        safe = jnp.maximum(ids, 0)
        source = lax.div(safe, cells)
        inner = safe - source * cells
        slab = lax.div(source, n_sub)
        block = (source - slab * n_sub) ^ q
        delta = slab - my_slab
        rim_at = n_sub * cells + block * (2 * RIM)
        column = jnp.where(
            delta == 0,
            block * cells + inner,
            jnp.where(delta < 0, rim_at + inner - (cells - RIM), rim_at + RIM + inner),
        )
        code = lax.shift_left(LANES + (column & (LANES - 1)), lax.shift_right_logical(column, 7))
        outs[r][order:, :] = jnp.where(ids >= 0, code, 0).astype(F32).astype(BF16)

    copies[1].wait()
    group = lax.shift_right_logical(lane, 5)
    chunks = []
    for q in range(4):
        want = 8 * (lane & (RIM - 1)) + 4 * lax.shift_right_logical(lane, 7) + ((group - q) & 3)
        hot = one_hot(row == jnp.broadcast_to(want.astype(F32).astype(BF16), (TILE, TILE)))
        chunk = jnp.dot(child[:, q * TILE : (q + 1) * TILE], hot, preferred_element_type=F32)
        chunks.append(chunk.astype(BF16))
    groups = jnp.broadcast_to(group[:, :LANES].astype(F32).astype(BF16), (order, LANES))
    copies[2].wait()
    total = None
    for j in range(4):
        turned = None
        for o in (j, j + 4):
            half = [x[:, o // 4 * LANES : (o // 4 + 1) * LANES] for x in chunks]
            part = jnp.dot(ops[o], by_group(groups, half, -j), preferred_element_type=F32)
            turned = part if turned is None else turned + part
        turned = turned if j == 0 else pltpu.roll(turned, LANES - RIM * j, 1)
        total = turned if total is None else total + turned
    total = total.astype(BF16)
    for r in range(n_sub):
        outs[r][:order, :] = total
    low, high = total[:, :RIM], total[:, cells - RIM :]
    even = lax.rem(my_slab, 2) == 0
    to_pair[...] = jnp.where(even, high, low)
    to_other[...] = jnp.where(even, low, high)


def up(child, ops, partners, n_sub):
    order = child.shape[0]
    cells = child.shape[1] // 8
    n_ops = partners.shape[0] // n_sub
    return pl.pallas_call(
        functools.partial(up_kernel, n_sub, cells),
        out_shape=[jax.ShapeDtypeStruct((order + n_ops, cells), BF16)] * n_sub
        + [jax.ShapeDtypeStruct((order, RIM), BF16)] * 2,
        in_specs=[HBM] * 3,
        out_specs=[VMEM] * (n_sub + 2),
        scratch_shapes=[
            pltpu.VMEM(child.shape, BF16),
            pltpu.VMEM(ops.shape, BF16),
            pltpu.VMEM(partners.shape, jnp.int32),
            pltpu.SemaphoreType.DMA((3,)),
        ],
        compiler_params=pltpu.CompilerParams(vmem_limit_bytes=16 << 20),
        cost_estimate=pl.CostEstimate(flops=1 << 30, bytes_accessed=2 << 20, transcendentals=0),
        name="up",
    )(*[pltpu.with_memory_space_constraint(x, pltpu.HBM) for x in (child, ops, partners)])


def spans_of(n_ops):
    return [(w, min(w + 32, n_ops)) for w in range(0, n_ops, 32)]


def pack(hit, n_ops):
    word = jnp.where(hit > 0.0, lax.shift_left(1, iota((n_ops, 1), 0) & 31), 0)
    return [jnp.sum(word[w:end]) for w, end in spans_of(n_ops)]


def each_bit(words, act, state):
    for i, word in enumerate(words):

        def step(carry, i=i):
            word, state = carry
            return word & (word - 1), act(32 * i + 31 - lax.clz(word & -word), state)

        state = lax.while_loop(lambda carry: carry[0] != 0, step, (word, state))[1]
    return state


def list_units(order, loads, n_ops, idx, code0, todo):
    cells = loads[0].shape[1]
    n_tiles = idx.shape[0]
    per = TILE // cells
    rows = iota((TILE, LANES), 0)
    code0[...] = lax.shift_left(LANES + (rows & (LANES - 1)), lax.shift_right_logical(rows, 7)).astype(F32).astype(BF16)
    hits = []
    for n in range(n_tiles):
        table = jnp.concatenate([x[order:, :].astype(F32) for x in loads[n * per : (n + 1) * per]], axis=1)
        idx[n, 0:n_ops, :] = table
        idx[n, n_ops : n_ops + 8, :] = jnp.zeros((8, TILE), F32)
        hits.append(jnp.max(table, axis=1, keepdims=True))
    count = jnp.int32(0)
    for n in range(n_tiles):

        def add(k, count, n=n):
            todo[count] = k * n_tiles + n
            return count + 1

        count = each_bit(pack(hits[n], n_ops), add, count)
    for a in range(GROUP):
        todo[count + a] = n_ops * n_tiles
    return hits, count, lax.div(count + GROUP - 1, GROUP)


def one_hots(row, base, first_tile, n_tiles):
    for t in range(first_tile, first_tile + n_tiles):
        scaled = (row * (4.0**-t)).astype(BF16)
        yield jnp.concatenate(
            [
                one_hot(base == jnp.broadcast_to(scaled[:, c : c + LANES], (TILE, LANES)))
                for c in range(0, TILE, LANES)
            ],
            axis=1,
        )


def pick_kernel(order, n_sub, *refs):
    loads, refs = refs[:n_sub], refs[n_sub:]
    ops_hbm, picked, ops, win, idx, code0, todo, sems = refs
    n_ops = ops.shape[0]
    n_tiles, k_tiles = idx.shape[0], win.shape[0]
    cells = loads[0].shape[1]
    for r in range(n_sub):
        win[r * cells // TILE, :, r * cells % TILE : r * cells % TILE + cells] = loads[r][:order, :]
    hits, count, trips = list_units(order, loads, n_ops, idx, code0, todo)

    used = jnp.where(iota((n_ops, 1), 0) == n_ops - 1, 1.0, functools.reduce(jnp.maximum, hits))
    used = pack(used, n_ops)

    def copy_in(k):
        return pltpu.make_async_copy(ops_hbm.at[k], ops.at[k], sems.at[k])

    def start(k, state):
        copy_in(k).start()
        return state

    def wait(k, state):
        copy_in(k).wait()
        return state

    each_bit(used, start, jnp.int32(0))

    def body(i, carry):
        base = code0[...]
        for a in range(GROUP):
            u = todo[GROUP * i + a]
            k = lax.div(u, n_tiles)
            row = idx[u - k * n_tiles, pl.ds(k, 1), :]
            total = None
            for t, hot in enumerate(one_hots(row, base, 0, k_tiles)):
                part = jnp.dot(win[t], hot, preferred_element_type=F32)
                total = part if total is None else total + part
            picked[GROUP * i + a] = total.astype(BF16)
        return carry

    lax.fori_loop(0, trips, body, 0)
    each_bit(used, wait, jnp.int32(0))


def apply_kernel(order, n_sub, *refs):
    loads, sides, refs = refs[:n_sub], refs[n_sub : 2 * n_sub], refs[2 * n_sub :]
    picked, ops, refs = refs[0], refs[1], refs[2:]
    outs, (win, idx, code0, acc, cols, todo) = refs[:n_sub], refs[n_sub:]
    n_ops = ops.shape[0]
    n_tiles, k_tiles = idx.shape[0], win.shape[0]
    cells = loads[0].shape[1]
    for i in range(0, n_sub, 2):
        at = i // 2 * LANES
        pair = jnp.concatenate([sides[i][...], sides[i + 1][...]], axis=1)
        win[at // TILE, :, at % TILE : at % TILE + LANES] = pair
    _, count, trips = list_units(order, loads, n_ops, idx, code0, todo)
    acc[...] = jnp.zeros_like(acc)

    def gather(i):
        base = code0[...]
        for a in range(GROUP):
            u = todo[GROUP * i + a]
            k = lax.div(u, n_tiles)
            row = idx[u - k * n_tiles, pl.ds(k, 1), :]
            total = None
            for t, hot in enumerate(one_hots(row, base, n_sub * cells // TILE, k_tiles)):
                part = jnp.dot(win[t], hot, preferred_element_type=F32)
                total = part if total is None else total + part
            cols[i & 1, a] = total.astype(BF16) + picked[GROUP * i + a]

    def apply(i):
        for a in range(GROUP):
            u = todo[GROUP * i + a]
            k = lax.div(u, n_tiles)
            acc[u - k * n_tiles] += jnp.dot(
                ops[jnp.minimum(k, n_ops - 1)], cols[i & 1, a], preferred_element_type=F32
            )

    def body(i, carry):
        apply(i - 1)
        gather(i)
        return carry

    @pl.when(trips > 0)
    def _():
        gather(0)
        lax.fori_loop(1, trips, body, 0)
        apply(trips - 1)

    for j, out in enumerate(outs):
        out[...] = acc[j * cells // TILE, :, j * cells % TILE : j * cells % TILE + cells].astype(out.dtype)


def m2l_sizes(loads, ops):
    n_sub, cells = len(loads), loads[0].shape[1]
    n_tiles = n_sub * cells // TILE
    return n_sub, cells, n_tiles, ops.shape[0] * n_tiles + GROUP


def pick(loads, ops, order):
    n_sub, cells, n_tiles, units = m2l_sizes(loads, ops)
    n_ops = ops.shape[0]
    return pl.pallas_call(
        functools.partial(pick_kernel, order, n_sub),
        out_shape=[jax.ShapeDtypeStruct((units, order, TILE), BF16), jax.ShapeDtypeStruct(ops.shape, BF16)],
        in_specs=[VMEM] * n_sub + [HBM],
        out_specs=[VMEM] * 2,
        scratch_shapes=[
            pltpu.VMEM((n_sub * cells // TILE, order, TILE), BF16),
            pltpu.VMEM((n_tiles, n_ops + 8, TILE), F32),
            pltpu.VMEM((TILE, LANES), BF16),
            pltpu.SMEM((units,), jnp.int32),
            pltpu.SemaphoreType.DMA((n_ops,)),
        ],
        compiler_params=pltpu.CompilerParams(vmem_limit_bytes=24 << 20),
        cost_estimate=pl.CostEstimate(flops=4 << 30, bytes_accessed=4 << 20, transcendentals=0),
        name="pick",
    )(*loads, pltpu.with_memory_space_constraint(ops, pltpu.HBM))


def apply_ops(loads, sides, picked, ops, order):
    n_sub, cells, n_tiles, units = m2l_sizes(loads, ops)
    n_ops = ops.shape[0]
    return pl.pallas_call(
        functools.partial(apply_kernel, order, n_sub),
        out_shape=[jax.ShapeDtypeStruct((order, cells), F32 if r == 0 else BF16) for r in range(n_sub)],
        in_specs=[VMEM] * (2 * n_sub + 2),
        out_specs=[VMEM] * n_sub,
        scratch_shapes=[
            pltpu.VMEM((n_sub * 2 * RIM // TILE, order, TILE), BF16),
            pltpu.VMEM((n_tiles, n_ops + 8, TILE), F32),
            pltpu.VMEM((TILE, LANES), BF16),
            pltpu.VMEM((n_tiles, order, TILE), F32),
            pltpu.VMEM((2, GROUP, order, TILE), BF16),
            pltpu.SMEM((units,), jnp.int32),
        ],
        compiler_params=pltpu.CompilerParams(vmem_limit_bytes=24 << 20),
        cost_estimate=pl.CostEstimate(flops=4 << 30, bytes_accessed=4 << 20, transcendentals=0),
        name="apply",
    )(*loads, *sides, picked, ops)


def down_kernel(n_parts, incoming, *refs):
    parts = refs[:n_parts]
    ops, out, stage, sem = refs[n_parts:]
    cells = incoming.shape[1]
    far = parts[0][...].astype(F32)
    for r in range(1, n_parts):
        far = far + parts[r][...].astype(F32)
    held = (incoming[...].astype(F32) + far).astype(BF16)
    order = held.shape[0]
    lane = iota((1, TILE), 1)
    row = iota((TILE, LANES), 0)
    base = 8 * (row & (RIM - 1)) + 4 * lax.shift_right_logical(row, 7)
    quarter = lax.shift_right_logical(row, 5)
    lane16 = lane.astype(F32).astype(BF16)
    groups = jnp.broadcast_to(lax.shift_right_logical(lane[:, :LANES], 5), (order, LANES))
    wide = held.astype(F32)
    turned = [held] + [pltpu.roll(wide, RIM * j, 1).astype(BF16) for j in range(1, 4)]
    made = [jnp.dot(ops[o], turned[o % 4], preferred_element_type=F32) for o in range(8)]
    copies = []
    for q in range(8 * cells // TILE):
        have = (base + ((quarter - q) & 3)).astype(F32).astype(BF16)
        hot = jnp.concatenate(
            [one_hot(have == jnp.broadcast_to(lane16[:, c : c + LANES], (TILE, LANES))) for c in (0, LANES)], axis=1
        )
        rest = jnp.concatenate([by_group(groups, made[4 * h : 4 * h + 4], -q) for h in range(2)], axis=1)
        total = None
        for _ in range(2):
            top = rest.astype(BF16)
            part = jnp.dot(top, hot, preferred_element_type=F32)
            total = part if total is None else total + part
            rest = rest - top.astype(F32)
        stage[q] = total
        copy = pltpu.make_async_copy(stage.at[q], out.at[:, q * TILE : (q + 1) * TILE], sem.at[q])
        copy.start()
        copies.append(copy)
    for copy in copies:
        copy.wait()


def down(incoming, parts, ops):
    order, cells = incoming.shape
    chunks = 8 * cells // TILE
    return pl.pallas_call(
        functools.partial(down_kernel, len(parts)),
        out_shape=jax.ShapeDtypeStruct((order, 8 * cells), F32),
        in_specs=[VMEM] * (len(parts) + 2),
        out_specs=pl.BlockSpec(memory_space=pl.ANY),
        scratch_shapes=[pltpu.VMEM((chunks, order, TILE), F32), pltpu.SemaphoreType.DMA((chunks,))],
        compiler_params=pltpu.CompilerParams(vmem_limit_bytes=16 << 20),
        cost_estimate=pl.CostEstimate(flops=1 << 30, bytes_accessed=2 << 20, transcendentals=0),
        name="down",
    )(incoming, *parts, ops)


def local(child_moments, incoming, m2m_ops, m2l_ops, l2l_ops, partners):
    order, cells = incoming.shape
    n_sub = lax.axis_size("sub")
    n_slab = lax.axis_size("slab")
    assert n_sub & (n_sub - 1) == 0 and n_slab % 2 == 0 and cells == LANES == 4 * RIM
    *sends, to_pair, to_other = up(child_moments, m2m_ops, partners, n_sub)
    got_other = lax.ppermute(to_other, "slab", [(i, ((i + 1) ^ 1) - 1) for i in range(1, n_slab - 1)])
    got_pair = lax.ppermute(to_pair, "slab", [(i, i ^ 1) for i in range(n_slab)])
    loads = [swap(sends[r], r, n_sub) for r in range(n_sub)]
    even = lax.axis_index("slab") % 2 == 0
    rim = jnp.concatenate(
        [jnp.where(even, got_other, got_pair), jnp.where(even, got_pair, got_other)], axis=1
    )
    sides = [swap(rim, r, n_sub) for r in range(n_sub)]
    picked, held_ops = pick(loads, m2l_ops, order)
    mine, *others = apply_ops(loads, sides, picked, held_ops, order)
    back = [swap(x, r + 1, n_sub) for r, x in reversed(list(enumerate(others)))]
    return down(incoming, [mine, *back], l2l_ops)


def solution(mesh):
    in_specs = (
        P(None, ("slab", "sub")),
        P(None, ("slab", "sub")),
        P(),
        P("sub", None, None),
        P(),
        P(None, ("slab", "sub")),
    )
    out_specs = P(None, ("slab", "sub"))
    return jax.shard_map(local, mesh=mesh, in_specs=in_specs, out_specs=out_specs, check_vma=False)
```

```python
import functools

import jax
import jax.numpy as jnp
from jax import lax
from jax.experimental import pallas as pl
from jax.experimental.pallas import tpu as pltpu
from jax.sharding import PartitionSpec as P


RIM = 32
TILE = 256
LANES = 128
GROUP = 8
VMEM = pl.BlockSpec(memory_space=pltpu.VMEM)
ANY = pl.BlockSpec(memory_space=pl.ANY)
HBM = pl.BlockSpec(memory_space=pltpu.HBM)
BF16 = jnp.bfloat16
F32 = jnp.float32


def swap(x, r, n):
    if r == 0:
        return x
    return lax.ppermute(x, "sub", [(i, i ^ r) for i in range(n)])


def one_hot(mask):
    return jnp.where(mask, jnp.ones((), BF16), jnp.zeros((), BF16))


def by_group(groups, parts, shift):
    out = parts[shift % 4]
    for g in range(1, 4):
        out = jnp.where(groups == jnp.full((), g, groups.dtype), parts[(g + shift) % 4], out)
    return out


def iota(shape, dim):
    return lax.broadcasted_iota(jnp.int32, shape, dim)


def up_kernel(n_sub, cells, child_hbm, ops_hbm, partners_hbm, *refs):
    outs, refs = refs[:n_sub], refs[n_sub:]
    to_pair, to_other, child, ops, partners, sems = refs
    copies = [
        pltpu.make_async_copy(src, dst, sems.at[i])
        for i, (src, dst) in enumerate([(partners_hbm, partners), (child_hbm, child), (ops_hbm, ops)])
    ]
    for copy in copies:
        copy.start()
    order = child.shape[0]
    lane = iota((1, TILE), 1)
    row = iota((TILE, TILE), 0).astype(F32).astype(BF16)

    copies[0].wait()
    n_ops = partners.shape[0] // n_sub
    my_slab = lax.axis_index("slab")
    me = lax.axis_index("sub")
    for r in range(n_sub):
        q = me ^ r
        ids = partners[pl.ds(pl.multiple_of(q * n_ops, n_ops), n_ops), :]
        safe = jnp.maximum(ids, 0)
        source = lax.div(safe, cells)
        inner = safe - source * cells
        slab = lax.div(source, n_sub)
        block = (source - slab * n_sub) ^ q
        delta = slab - my_slab
        rim_at = n_sub * cells + block * (2 * RIM)
        column = jnp.where(
            delta == 0,
            block * cells + inner,
            jnp.where(delta < 0, rim_at + inner - (cells - RIM), rim_at + RIM + inner),
        )
        code = lax.shift_left(LANES + (column & (LANES - 1)), lax.shift_right_logical(column, 7))
        outs[r][order:, :] = jnp.where(ids >= 0, code, 0).astype(F32).astype(BF16)

    copies[1].wait()
    group = lax.shift_right_logical(lane, 5)
    chunks = []
    for q in range(4):
        want = 8 * (lane & (RIM - 1)) + 4 * lax.shift_right_logical(lane, 7) + ((group - q) & 3)
        hot = one_hot(row == jnp.broadcast_to(want.astype(F32).astype(BF16), (TILE, TILE)))
        chunk = jnp.dot(child[:, q * TILE : (q + 1) * TILE], hot, preferred_element_type=F32)
        chunks.append(chunk.astype(BF16))
    groups = jnp.broadcast_to(group[:, :LANES].astype(F32).astype(BF16), (order, LANES))
    copies[2].wait()
    total = None
    for j in range(4):
        turned = None
        for o in (j, j + 4):
            half = [x[:, o // 4 * LANES : (o // 4 + 1) * LANES] for x in chunks]
            part = jnp.dot(ops[o], by_group(groups, half, -j), preferred_element_type=F32)
            turned = part if turned is None else turned + part
        turned = turned if j == 0 else pltpu.roll(turned, LANES - RIM * j, 1)
        total = turned if total is None else total + turned
    total = total.astype(BF16)
    for r in range(n_sub):
        outs[r][:order, :] = total
    low, high = total[:, :RIM], total[:, cells - RIM :]
    even = lax.rem(my_slab, 2) == 0
    to_pair[...] = jnp.where(even, high, low)
    to_other[...] = jnp.where(even, low, high)


def up(child, ops, partners, n_sub):
    order = child.shape[0]
    cells = child.shape[1] // 8
    n_ops = partners.shape[0] // n_sub
    return pl.pallas_call(
        functools.partial(up_kernel, n_sub, cells),
        out_shape=[jax.ShapeDtypeStruct((order + n_ops, cells), BF16)] * n_sub
        + [jax.ShapeDtypeStruct((order, RIM), BF16)] * 2,
        in_specs=[HBM] * 3,
        out_specs=[VMEM] * (n_sub + 2),
        scratch_shapes=[
            pltpu.VMEM(child.shape, BF16),
            pltpu.VMEM(ops.shape, BF16),
            pltpu.VMEM(partners.shape, jnp.int32),
            pltpu.SemaphoreType.DMA((3,)),
        ],
        compiler_params=pltpu.CompilerParams(vmem_limit_bytes=16 << 20),
        cost_estimate=pl.CostEstimate(flops=1 << 30, bytes_accessed=2 << 20, transcendentals=0),
        name="up",
    )(*[pltpu.with_memory_space_constraint(x, pltpu.HBM) for x in (child, ops, partners)])


def spans_of(n_ops):
    return [(w, min(w + 32, n_ops)) for w in range(0, n_ops, 32)]


def pack(hit, n_ops):
    word = jnp.where(hit > 0.0, lax.shift_left(1, iota((n_ops, 1), 0) & 31), 0)
    return [jnp.sum(word[w:end]) for w, end in spans_of(n_ops)]


def each_bit(words, act, state):
    for i, word in enumerate(words):

        def step(carry, i=i):
            word, state = carry
            return word & (word - 1), act(32 * i + 31 - lax.clz(word & -word), state)

        state = lax.while_loop(lambda carry: carry[0] != 0, step, (word, state))[1]
    return state


def list_units(order, loads, n_ops, idx, code0, todo):
    cells = loads[0].shape[1]
    n_tiles = idx.shape[0]
    per = TILE // cells
    rows = iota((TILE, LANES), 0)
    code0[...] = lax.shift_left(LANES + (rows & (LANES - 1)), lax.shift_right_logical(rows, 7)).astype(F32).astype(BF16)
    hits = []
    for n in range(n_tiles):
        table = jnp.concatenate([x[order:, :].astype(F32) for x in loads[n * per : (n + 1) * per]], axis=1)
        idx[n, 0:n_ops, :] = table
        idx[n, n_ops : n_ops + 8, :] = jnp.zeros((8, TILE), F32)
        hits.append(jnp.max(table, axis=1, keepdims=True))
    count = jnp.int32(0)
    for n in range(n_tiles):

        def add(k, count, n=n):
            todo[count] = k * n_tiles + n
            return count + 1

        count = each_bit(pack(hits[n], n_ops), add, count)
    for a in range(GROUP):
        todo[count + a] = n_ops * n_tiles
    return hits, count, lax.div(count + GROUP - 1, GROUP)


def one_hots(row, base, first_tile, n_tiles):
    for t in range(first_tile, first_tile + n_tiles):
        scaled = (row * (4.0**-t)).astype(BF16)
        yield jnp.concatenate(
            [
                one_hot(base == jnp.broadcast_to(scaled[:, c : c + LANES], (TILE, LANES)))
                for c in range(0, TILE, LANES)
            ],
            axis=1,
        )


def pick_kernel(order, n_sub, *refs):
    loads, refs = refs[:n_sub], refs[n_sub:]
    ops_hbm, picked, ops, win, idx, code0, todo, sems = refs
    n_ops = ops.shape[0]
    n_tiles, k_tiles = idx.shape[0], win.shape[0]
    cells = loads[0].shape[1]
    for r in range(n_sub):
        win[r * cells // TILE, :, r * cells % TILE : r * cells % TILE + cells] = loads[r][:order, :]
    hits, _, trips = list_units(order, loads, n_ops, idx, code0, todo)

    used = jnp.where(iota((n_ops, 1), 0) == n_ops - 1, 1.0, functools.reduce(jnp.maximum, hits))
    used = pack(used, n_ops)

    def copy_in(k):
        return pltpu.make_async_copy(ops_hbm.at[k], ops.at[k], sems.at[k])

    def start(k, state):
        copy_in(k).start()
        return state

    def wait(k, state):
        copy_in(k).wait()
        return state

    each_bit(used, start, jnp.int32(0))

    def body(i, carry):
        base = code0[...]
        for a in range(GROUP):
            u = todo[GROUP * i + a]
            k = lax.div(u, n_tiles)
            row = idx[u - k * n_tiles, pl.ds(k, 1), :]
            total = None
            for t, hot in enumerate(one_hots(row, base, 0, k_tiles)):
                part = jnp.dot(win[t], hot, preferred_element_type=F32)
                total = part if total is None else total + part
            picked[GROUP * i + a] = total.astype(BF16)
        return carry

    lax.fori_loop(0, trips, body, 0)
    each_bit(used, wait, jnp.int32(0))


def apply_kernel(order, n_sub, *refs):
    loads, sides, refs = refs[:n_sub], refs[n_sub : 2 * n_sub], refs[2 * n_sub :]
    picked, ops, refs = refs[0], refs[1], refs[2:]
    outs, (win, idx, code0, acc, cols, todo) = refs[:n_sub], refs[n_sub:]
    n_ops = ops.shape[0]
    n_tiles, k_tiles = idx.shape[0], win.shape[0]
    cells = loads[0].shape[1]
    for i in range(0, n_sub, 2):
        at = i // 2 * LANES
        pair = jnp.concatenate([sides[i][...], sides[i + 1][...]], axis=1)
        win[at // TILE, :, at % TILE : at % TILE + LANES] = pair
    _, _, trips = list_units(order, loads, n_ops, idx, code0, todo)
    acc[...] = jnp.zeros_like(acc)

    def gather(i):
        base = code0[...]
        for a in range(GROUP):
            u = todo[GROUP * i + a]
            k = lax.div(u, n_tiles)
            row = idx[u - k * n_tiles, pl.ds(k, 1), :]
            total = None
            for t, hot in enumerate(one_hots(row, base, n_sub * cells // TILE, k_tiles)):
                part = jnp.dot(win[t], hot, preferred_element_type=F32)
                total = part if total is None else total + part
            cols[i & 1, a] = total.astype(BF16) + picked[GROUP * i + a]

    def apply(i):
        for a in range(GROUP):
            u = todo[GROUP * i + a]
            k = lax.div(u, n_tiles)
            acc[u - k * n_tiles] += jnp.dot(
                ops[jnp.minimum(k, n_ops - 1)], cols[i & 1, a], preferred_element_type=F32
            )

    def body(i, carry):
        apply(i - 1)
        gather(i)
        return carry

    @pl.when(trips > 0)
    def _():
        gather(0)
        lax.fori_loop(1, trips, body, 0)
        apply(trips - 1)

    for j, out in enumerate(outs):
        out[...] = acc[j * cells // TILE, :, j * cells % TILE : j * cells % TILE + cells].astype(out.dtype)


def m2l_sizes(loads, ops):
    n_sub, cells = len(loads), loads[0].shape[1]
    n_tiles = n_sub * cells // TILE
    return n_sub, cells, n_tiles, ops.shape[0] * n_tiles + GROUP


def pick(loads, ops, order):
    n_sub, cells, n_tiles, units = m2l_sizes(loads, ops)
    n_ops = ops.shape[0]
    return pl.pallas_call(
        functools.partial(pick_kernel, order, n_sub),
        out_shape=[jax.ShapeDtypeStruct((units, order, TILE), BF16), jax.ShapeDtypeStruct(ops.shape, BF16)],
        in_specs=[VMEM] * n_sub + [HBM],
        out_specs=[VMEM] * 2,
        scratch_shapes=[
            pltpu.VMEM((n_sub * cells // TILE, order, TILE), BF16),
            pltpu.VMEM((n_tiles, n_ops + 8, TILE), F32),
            pltpu.VMEM((TILE, LANES), BF16),
            pltpu.SMEM((units,), jnp.int32),
            pltpu.SemaphoreType.DMA((n_ops,)),
        ],
        compiler_params=pltpu.CompilerParams(vmem_limit_bytes=24 << 20),
        cost_estimate=pl.CostEstimate(flops=4 << 30, bytes_accessed=4 << 20, transcendentals=0),
        name="pick",
    )(*loads, pltpu.with_memory_space_constraint(ops, pltpu.HBM))


def apply_ops(loads, sides, picked, ops, order):
    n_sub, cells, n_tiles, units = m2l_sizes(loads, ops)
    n_ops = ops.shape[0]
    return pl.pallas_call(
        functools.partial(apply_kernel, order, n_sub),
        out_shape=[jax.ShapeDtypeStruct((order, cells), F32 if r == 0 else BF16) for r in range(n_sub)],
        in_specs=[VMEM] * (2 * n_sub + 2),
        out_specs=[VMEM] * n_sub,
        scratch_shapes=[
            pltpu.VMEM((n_sub * 2 * RIM // TILE, order, TILE), BF16),
            pltpu.VMEM((n_tiles, n_ops + 8, TILE), F32),
            pltpu.VMEM((TILE, LANES), BF16),
            pltpu.VMEM((n_tiles, order, TILE), F32),
            pltpu.VMEM((2, GROUP, order, TILE), BF16),
            pltpu.SMEM((units,), jnp.int32),
        ],
        compiler_params=pltpu.CompilerParams(vmem_limit_bytes=24 << 20),
        cost_estimate=pl.CostEstimate(flops=4 << 30, bytes_accessed=4 << 20, transcendentals=0),
        name="apply",
    )(*loads, *sides, picked, ops)


def down_kernel(n_parts, incoming, *refs):
    parts = refs[:n_parts]
    ops, out, stage, sem = refs[n_parts:]
    cells = incoming.shape[1]
    far = parts[0][...].astype(F32)
    for r in range(1, n_parts):
        far = far + parts[r][...].astype(F32)
    held = (incoming[...].astype(F32) + far).astype(BF16)
    order = held.shape[0]
    lane = iota((1, TILE), 1)
    row = iota((TILE, LANES), 0)
    base = 8 * (row & (RIM - 1)) + 4 * lax.shift_right_logical(row, 7)
    quarter = lax.shift_right_logical(row, 5)
    lane16 = lane.astype(F32).astype(BF16)
    groups = jnp.broadcast_to(lax.shift_right_logical(lane[:, :LANES], 5), (order, LANES))
    wide = held.astype(F32)
    turned = [held] + [pltpu.roll(wide, RIM * j, 1).astype(BF16) for j in range(1, 4)]
    made = [jnp.dot(ops[o], turned[o % 4], preferred_element_type=F32) for o in range(8)]
    copies = []
    for q in range(8 * cells // TILE):
        have = (base + ((quarter - q) & 3)).astype(F32).astype(BF16)
        hot = jnp.concatenate(
            [one_hot(have == jnp.broadcast_to(lane16[:, c : c + LANES], (TILE, LANES))) for c in (0, LANES)], axis=1
        )
        rest = jnp.concatenate([by_group(groups, made[4 * h : 4 * h + 4], -q) for h in range(2)], axis=1)
        total = None
        for _ in range(2):
            top = rest.astype(BF16)
            part = jnp.dot(top, hot, preferred_element_type=F32)
            total = part if total is None else total + part
            rest = rest - top.astype(F32)
        stage[q] = total
        copy = pltpu.make_async_copy(stage.at[q], out.at[:, q * TILE : (q + 1) * TILE], sem.at[q])
        copy.start()
        copies.append(copy)
    for copy in copies:
        copy.wait()


def down(incoming, parts, ops):
    order, cells = incoming.shape
    chunks = 8 * cells // TILE
    return pl.pallas_call(
        functools.partial(down_kernel, len(parts)),
        out_shape=jax.ShapeDtypeStruct((order, 8 * cells), F32),
        in_specs=[VMEM] * (len(parts) + 2),
        out_specs=pl.BlockSpec(memory_space=pl.ANY),
        scratch_shapes=[pltpu.VMEM((chunks, order, TILE), F32), pltpu.SemaphoreType.DMA((chunks,))],
        compiler_params=pltpu.CompilerParams(vmem_limit_bytes=16 << 20),
        cost_estimate=pl.CostEstimate(flops=1 << 30, bytes_accessed=2 << 20, transcendentals=0),
        name="down",
    )(incoming, *parts, ops)


def far_field(child_moments, incoming, m2m_ops, m2l_ops, l2l_ops, partners):
    order, cells = incoming.shape
    n_sub = lax.axis_size("sub")
    n_slab = lax.axis_size("slab")
    assert n_sub & (n_sub - 1) == 0 and n_slab % 2 == 0 and cells == LANES == 4 * RIM
    *sends, to_pair, to_other = up(child_moments, m2m_ops, partners, n_sub)
    got_pair = lax.ppermute(to_pair, "slab", [(i, i ^ 1) for i in range(n_slab)])
    got_other = lax.ppermute(to_other, "slab", [(i, ((i + 1) ^ 1) - 1) for i in range(1, n_slab - 1)])
    loads = [swap(sends[r], r, n_sub) for r in range(n_sub)]
    even = lax.axis_index("slab") % 2 == 0
    rim = jnp.concatenate(
        [jnp.where(even, got_other, got_pair), jnp.where(even, got_pair, got_other)], axis=1
    )
    sides = [swap(rim, r, n_sub) for r in range(n_sub)]
    picked, held_ops = pick(loads, m2l_ops, order)
    mine, *others = apply_ops(loads, sides, picked, held_ops, order)
    back = [swap(x, r + 1, n_sub) for r, x in reversed(list(enumerate(others)))]
    return down(incoming, [mine, *back], l2l_ops)


def solution(mesh):
    in_specs = (
        P(None, ("slab", "sub")),
        P(None, ("slab", "sub")),
        P(),
        P("sub", None, None),
        P(),
        P(None, ("slab", "sub")),
    )
    out_specs = P(None, ("slab", "sub"))
    return jax.shard_map(far_field, mesh=mesh, in_specs=in_specs, out_specs=out_specs, check_vma=False)
```

```python
import functools

import jax
import jax.numpy as jnp
from jax import lax
from jax.experimental import pallas as pl
from jax.experimental.pallas import tpu as pltpu
from jax.sharding import PartitionSpec as P


RIM = 32
TILE = 256
LANES = 128
GROUP = 8
VMEM = pl.BlockSpec(memory_space=pltpu.VMEM)
ANY = pl.BlockSpec(memory_space=pl.ANY)
HBM = pl.BlockSpec(memory_space=pltpu.HBM)
BF16 = jnp.bfloat16
F32 = jnp.float32


def swap(x, r, n):
    if r == 0:
        return x
    return lax.ppermute(x, "sub", [(i, i ^ r) for i in range(n)])


def one_hot(mask):
    return jnp.where(mask, jnp.ones((), BF16), jnp.zeros((), BF16))


def by_group(groups, parts, shift):
    out = parts[shift % 4]
    for g in range(1, 4):
        out = jnp.where(groups == jnp.full((), g, groups.dtype), parts[(g + shift) % 4], out)
    return out


def iota(shape, dim):
    return lax.broadcasted_iota(jnp.int32, shape, dim)


def up_kernel(n_sub, cells, child_hbm, ops_hbm, partners_hbm, *refs):
    outs, refs = refs[:n_sub], refs[n_sub:]
    to_pair, to_other, child, ops, partners, sems = refs
    copies = [
        pltpu.make_async_copy(src, dst, sems.at[i])
        for i, (src, dst) in enumerate([(partners_hbm, partners), (child_hbm, child), (ops_hbm, ops)])
    ]
    for copy in copies:
        copy.start()
    order = child.shape[0]
    lane = iota((1, TILE), 1)
    row = iota((TILE, TILE), 0).astype(F32).astype(BF16)

    copies[0].wait()
    n_ops = partners.shape[0] // n_sub
    my_slab = lax.axis_index("slab")
    me = lax.axis_index("sub")
    for r in range(n_sub):
        q = me ^ r
        ids = partners[pl.ds(pl.multiple_of(q * n_ops, n_ops), n_ops), :]
        safe = jnp.maximum(ids, 0)
        source = lax.div(safe, cells)
        inner = safe - source * cells
        slab = lax.div(source, n_sub)
        block = (source - slab * n_sub) ^ q
        delta = slab - my_slab
        rim_at = n_sub * cells + block * (2 * RIM)
        column = jnp.where(
            delta == 0,
            block * cells + inner,
            jnp.where(delta < 0, rim_at + inner - (cells - RIM), rim_at + RIM + inner),
        )
        code = lax.shift_left(LANES + (column & (LANES - 1)), lax.shift_right_logical(column, 7))
        outs[r][order:, :] = jnp.where(ids >= 0, code, 0).astype(F32).astype(BF16)

    copies[1].wait()
    group = lax.shift_right_logical(lane, 5)
    chunks = []
    for q in range(4):
        want = 8 * (lane & (RIM - 1)) + 4 * lax.shift_right_logical(lane, 7) + ((group - q) & 3)
        hot = one_hot(row == jnp.broadcast_to(want.astype(F32).astype(BF16), (TILE, TILE)))
        chunk = jnp.dot(child[:, q * TILE : (q + 1) * TILE], hot, preferred_element_type=F32)
        chunks.append(chunk.astype(BF16))
    groups = jnp.broadcast_to(group[:, :LANES].astype(F32).astype(BF16), (order, LANES))
    copies[2].wait()
    total = None
    for j in range(4):
        turned = None
        for o in (j, j + 4):
            half = [x[:, o // 4 * LANES : (o // 4 + 1) * LANES] for x in chunks]
            part = jnp.dot(ops[o], by_group(groups, half, -j), preferred_element_type=F32)
            turned = part if turned is None else turned + part
        turned = turned if j == 0 else pltpu.roll(turned, LANES - RIM * j, 1)
        total = turned if total is None else total + turned
    total = total.astype(BF16)
    for r in range(n_sub):
        outs[r][:order, :] = total
    low, high = total[:, :RIM], total[:, cells - RIM :]
    even = lax.rem(my_slab, 2) == 0
    to_pair[...] = jnp.where(even, high, low)
    to_other[...] = jnp.where(even, low, high)


def up(child, ops, partners, n_sub):
    order = child.shape[0]
    cells = child.shape[1] // 8
    n_ops = partners.shape[0] // n_sub
    return pl.pallas_call(
        functools.partial(up_kernel, n_sub, cells),
        out_shape=[jax.ShapeDtypeStruct((order + n_ops, cells), BF16)] * n_sub
        + [jax.ShapeDtypeStruct((order, RIM), BF16)] * 2,
        in_specs=[HBM] * 3,
        out_specs=[VMEM] * (n_sub + 2),
        scratch_shapes=[
            pltpu.VMEM(child.shape, BF16),
            pltpu.VMEM(ops.shape, BF16),
            pltpu.VMEM(partners.shape, jnp.int32),
            pltpu.SemaphoreType.DMA((3,)),
        ],
        compiler_params=pltpu.CompilerParams(vmem_limit_bytes=16 << 20),
        cost_estimate=pl.CostEstimate(flops=1 << 30, bytes_accessed=2 << 20, transcendentals=0),
        name="up",
    )(*[pltpu.with_memory_space_constraint(x, pltpu.HBM) for x in (child, ops, partners)])


def spans_of(n_ops):
    return [(w, min(w + 32, n_ops)) for w in range(0, n_ops, 32)]


def pack(hit, n_ops):
    word = jnp.where(hit > 0.0, lax.shift_left(1, iota((n_ops, 1), 0) & 31), 0)
    return [jnp.sum(word[w:end]) for w, end in spans_of(n_ops)]


def each_bit(words, act, state):
    for i, word in enumerate(words):

        def step(carry, i=i):
            word, state = carry
            return word & (word - 1), act(32 * i + 31 - lax.clz(word & -word), state)

        state = lax.while_loop(lambda carry: carry[0] != 0, step, (word, state))[1]
    return state


def list_units(order, loads, n_ops, idx, code0, todo):
    cells = loads[0].shape[1]
    n_tiles = idx.shape[0]
    per = TILE // cells
    rows = iota((TILE, LANES), 0)
    code0[...] = lax.shift_left(LANES + (rows & (LANES - 1)), lax.shift_right_logical(rows, 7)).astype(F32).astype(BF16)
    hits = []
    for n in range(n_tiles):
        table = jnp.concatenate([x[order:, :].astype(F32) for x in loads[n * per : (n + 1) * per]], axis=1)
        idx[n, 0:n_ops, :] = table
        idx[n, n_ops : n_ops + 8, :] = jnp.zeros((8, TILE), F32)
        hits.append(jnp.max(table, axis=1, keepdims=True))
    count = jnp.int32(0)
    for n in range(n_tiles):

        def add(k, count, n=n):
            todo[count] = k * n_tiles + n
            return count + 1

        count = each_bit(pack(hits[n], n_ops), add, count)
    for a in range(GROUP):
        todo[count + a] = n_ops * n_tiles
    full = lax.div(count, GROUP)
    rest = count - full * GROUP
    short = jnp.logical_and(rest > 0, rest <= GROUP // 2)
    return hits, jnp.where(rest > GROUP // 2, full + 1, full), short


def one_hots(row, base, first_tile, n_tiles):
    for t in range(first_tile, first_tile + n_tiles):
        scaled = (row * (4.0**-t)).astype(BF16)
        yield jnp.concatenate(
            [
                one_hot(base == jnp.broadcast_to(scaled[:, c : c + LANES], (TILE, LANES)))
                for c in range(0, TILE, LANES)
            ],
            axis=1,
        )


def pick_kernel(order, n_sub, *refs):
    loads, refs = refs[:n_sub], refs[n_sub:]
    ops_hbm, picked, ops, win, idx, code0, todo, sems = refs
    n_ops = ops.shape[0]
    n_tiles, k_tiles = idx.shape[0], win.shape[0]
    cells = loads[0].shape[1]
    for r in range(n_sub):
        win[r * cells // TILE, :, r * cells % TILE : r * cells % TILE + cells] = loads[r][:order, :]
    hits, full, short = list_units(order, loads, n_ops, idx, code0, todo)

    used = jnp.where(iota((n_ops, 1), 0) == n_ops - 1, 1.0, functools.reduce(jnp.maximum, hits))
    used = pack(used, n_ops)

    def copy_in(k):
        return pltpu.make_async_copy(ops_hbm.at[k], ops.at[k], sems.at[k])

    def start(k, state):
        copy_in(k).start()
        return state

    def wait(k, state):
        copy_in(k).wait()
        return state

    each_bit(used, start, jnp.int32(0))

    def gather(i, size):
        base = code0[...]
        for a in range(size):
            u = todo[GROUP * i + a]
            k = lax.div(u, n_tiles)
            row = idx[u - k * n_tiles, pl.ds(k, 1), :]
            total = None
            for t, hot in enumerate(one_hots(row, base, 0, k_tiles)):
                part = jnp.dot(win[t], hot, preferred_element_type=F32)
                total = part if total is None else total + part
            picked[GROUP * i + a] = total.astype(BF16)

    def body(i, carry):
        gather(i, GROUP)
        return carry

    lax.fori_loop(0, full, body, 0)

    @pl.when(short)
    def _():
        gather(full, GROUP // 2)

    each_bit(used, wait, jnp.int32(0))


def apply_kernel(order, n_sub, *refs):
    loads, sides, refs = refs[:n_sub], refs[n_sub : 2 * n_sub], refs[2 * n_sub :]
    picked, ops, refs = refs[0], refs[1], refs[2:]
    outs, (win, idx, code0, acc, cols, todo) = refs[:n_sub], refs[n_sub:]
    n_ops = ops.shape[0]
    n_tiles, k_tiles = idx.shape[0], win.shape[0]
    cells = loads[0].shape[1]
    for i in range(0, n_sub, 2):
        at = i // 2 * LANES
        pair = jnp.concatenate([sides[i][...], sides[i + 1][...]], axis=1)
        win[at // TILE, :, at % TILE : at % TILE + LANES] = pair
    _, full, short = list_units(order, loads, n_ops, idx, code0, todo)
    acc[...] = jnp.zeros_like(acc)

    def gather(i, size):
        base = code0[...]
        for a in range(size):
            u = todo[GROUP * i + a]
            k = lax.div(u, n_tiles)
            row = idx[u - k * n_tiles, pl.ds(k, 1), :]
            total = None
            for t, hot in enumerate(one_hots(row, base, n_sub * cells // TILE, k_tiles)):
                part = jnp.dot(win[t], hot, preferred_element_type=F32)
                total = part if total is None else total + part
            cols[i & 1, a] = total.astype(BF16) + picked[GROUP * i + a]

    def apply(i, size):
        for a in range(size):
            u = todo[GROUP * i + a]
            k = lax.div(u, n_tiles)
            acc[u - k * n_tiles] += jnp.dot(
                ops[jnp.minimum(k, n_ops - 1)], cols[i & 1, a], preferred_element_type=F32
            )

    def body(i, carry):
        apply(i - 1, GROUP)
        gather(i, GROUP)
        return carry

    @pl.when(full > 0)
    def _():
        gather(0, GROUP)
        lax.fori_loop(1, full, body, 0)

    @pl.when(jnp.logical_and(full > 0, jnp.logical_not(short)))
    def _():
        apply(full - 1, GROUP)

    @pl.when(jnp.logical_and(full > 0, short))
    def _():
        apply(full - 1, GROUP)
        gather(full, GROUP // 2)

    @pl.when(jnp.logical_and(full == 0, short))
    def _():
        gather(full, GROUP // 2)

    @pl.when(short)
    def _():
        apply(full, GROUP // 2)

    for j, out in enumerate(outs):
        out[...] = acc[j * cells // TILE, :, j * cells % TILE : j * cells % TILE + cells].astype(out.dtype)


def m2l_sizes(loads, ops):
    n_sub, cells = len(loads), loads[0].shape[1]
    n_tiles = n_sub * cells // TILE
    return n_sub, cells, n_tiles, ops.shape[0] * n_tiles + GROUP


def pick(loads, ops, order):
    n_sub, cells, n_tiles, units = m2l_sizes(loads, ops)
    n_ops = ops.shape[0]
    return pl.pallas_call(
        functools.partial(pick_kernel, order, n_sub),
        out_shape=[jax.ShapeDtypeStruct((units, order, TILE), BF16), jax.ShapeDtypeStruct(ops.shape, BF16)],
        in_specs=[VMEM] * n_sub + [HBM],
        out_specs=[VMEM] * 2,
        scratch_shapes=[
            pltpu.VMEM((n_sub * cells // TILE, order, TILE), BF16),
            pltpu.VMEM((n_tiles, n_ops + 8, TILE), F32),
            pltpu.VMEM((TILE, LANES), BF16),
            pltpu.SMEM((units,), jnp.int32),
            pltpu.SemaphoreType.DMA((n_ops,)),
        ],
        compiler_params=pltpu.CompilerParams(vmem_limit_bytes=24 << 20),
        cost_estimate=pl.CostEstimate(flops=4 << 30, bytes_accessed=4 << 20, transcendentals=0),
        name="pick",
    )(*loads, pltpu.with_memory_space_constraint(ops, pltpu.HBM))


def apply_ops(loads, sides, picked, ops, order):
    n_sub, cells, n_tiles, units = m2l_sizes(loads, ops)
    n_ops = ops.shape[0]
    return pl.pallas_call(
        functools.partial(apply_kernel, order, n_sub),
        out_shape=[jax.ShapeDtypeStruct((order, cells), F32 if r == 0 else BF16) for r in range(n_sub)],
        in_specs=[VMEM] * (2 * n_sub + 2),
        out_specs=[VMEM] * n_sub,
        scratch_shapes=[
            pltpu.VMEM((n_sub * 2 * RIM // TILE, order, TILE), BF16),
            pltpu.VMEM((n_tiles, n_ops + 8, TILE), F32),
            pltpu.VMEM((TILE, LANES), BF16),
            pltpu.VMEM((n_tiles, order, TILE), F32),
            pltpu.VMEM((2, GROUP, order, TILE), BF16),
            pltpu.SMEM((units,), jnp.int32),
        ],
        compiler_params=pltpu.CompilerParams(vmem_limit_bytes=24 << 20),
        cost_estimate=pl.CostEstimate(flops=4 << 30, bytes_accessed=4 << 20, transcendentals=0),
        name="apply",
    )(*loads, *sides, picked, ops)


def down_kernel(n_parts, incoming, *refs):
    parts = refs[:n_parts]
    ops, out, stage, sem = refs[n_parts:]
    cells = incoming.shape[1]
    far = parts[0][...].astype(F32)
    for r in range(1, n_parts):
        far = far + parts[r][...].astype(F32)
    held = (incoming[...].astype(F32) + far).astype(BF16)
    order = held.shape[0]
    lane = iota((1, TILE), 1)
    row = iota((TILE, LANES), 0)
    base = 8 * (row & (RIM - 1)) + 4 * lax.shift_right_logical(row, 7)
    quarter = lax.shift_right_logical(row, 5)
    lane16 = lane.astype(F32).astype(BF16)
    groups = jnp.broadcast_to(lax.shift_right_logical(lane[:, :LANES], 5), (order, LANES))
    wide = held.astype(F32)
    turned = [held] + [pltpu.roll(wide, RIM * j, 1).astype(BF16) for j in range(1, 4)]
    made = [jnp.dot(ops[o], turned[o % 4], preferred_element_type=F32) for o in range(8)]
    copies = []
    for q in range(8 * cells // TILE):
        have = (base + ((quarter - q) & 3)).astype(F32).astype(BF16)
        hot = jnp.concatenate(
            [one_hot(have == jnp.broadcast_to(lane16[:, c : c + LANES], (TILE, LANES))) for c in (0, LANES)], axis=1
        )
        rest = jnp.concatenate([by_group(groups, made[4 * h : 4 * h + 4], -q) for h in range(2)], axis=1)
        total = None
        for _ in range(2):
            top = rest.astype(BF16)
            part = jnp.dot(top, hot, preferred_element_type=F32)
            total = part if total is None else total + part
            rest = rest - top.astype(F32)
        stage[q] = total
        copy = pltpu.make_async_copy(stage.at[q], out.at[:, q * TILE : (q + 1) * TILE], sem.at[q])
        copy.start()
        copies.append(copy)
    for copy in copies:
        copy.wait()


def down(incoming, parts, ops):
    order, cells = incoming.shape
    chunks = 8 * cells // TILE
    return pl.pallas_call(
        functools.partial(down_kernel, len(parts)),
        out_shape=jax.ShapeDtypeStruct((order, 8 * cells), F32),
        in_specs=[VMEM] * (len(parts) + 2),
        out_specs=pl.BlockSpec(memory_space=pl.ANY),
        scratch_shapes=[pltpu.VMEM((chunks, order, TILE), F32), pltpu.SemaphoreType.DMA((chunks,))],
        compiler_params=pltpu.CompilerParams(vmem_limit_bytes=16 << 20),
        cost_estimate=pl.CostEstimate(flops=1 << 30, bytes_accessed=2 << 20, transcendentals=0),
        name="down",
    )(incoming, *parts, ops)


def far_field(child_moments, incoming, m2m_ops, m2l_ops, l2l_ops, partners):
    order, cells = incoming.shape
    n_sub = lax.axis_size("sub")
    n_slab = lax.axis_size("slab")
    assert n_sub & (n_sub - 1) == 0 and n_slab % 2 == 0 and cells == LANES == 4 * RIM
    *sends, to_pair, to_other = up(child_moments, m2m_ops, partners, n_sub)
    got_pair = lax.ppermute(to_pair, "slab", [(i, i ^ 1) for i in range(n_slab)])
    got_other = lax.ppermute(to_other, "slab", [(i, ((i + 1) ^ 1) - 1) for i in range(1, n_slab - 1)])
    loads = [swap(sends[r], r, n_sub) for r in range(n_sub)]
    even = lax.axis_index("slab") % 2 == 0
    rim = jnp.concatenate(
        [jnp.where(even, got_other, got_pair), jnp.where(even, got_pair, got_other)], axis=1
    )
    sides = [swap(rim, r, n_sub) for r in range(n_sub)]
    picked, held_ops = pick(loads, m2l_ops, order)
    mine, *others = apply_ops(loads, sides, picked, held_ops, order)
    back = [swap(x, r + 1, n_sub) for r, x in reversed(list(enumerate(others)))]
    return down(incoming, [mine, *back], l2l_ops)


def solution(mesh):
    in_specs = (
        P(None, ("slab", "sub")),
        P(None, ("slab", "sub")),
        P(),
        P("sub", None, None),
        P(),
        P(None, ("slab", "sub")),
    )
    out_specs = P(None, ("slab", "sub"))
    return jax.shard_map(far_field, mesh=mesh, in_specs=in_specs, out_specs=out_specs, check_vma=False)
```

```python
import functools

import jax
import jax.numpy as jnp
from jax import lax
from jax.experimental import pallas as pl
from jax.experimental.pallas import tpu as pltpu
from jax.sharding import PartitionSpec as P


RIM = 32
TILE = 256
LANES = 128
GROUP = 8
FETCHES = 4
VMEM = pl.BlockSpec(memory_space=pltpu.VMEM)
ANY = pl.BlockSpec(memory_space=pl.ANY)
HBM = pl.BlockSpec(memory_space=pltpu.HBM)
BF16 = jnp.bfloat16
F32 = jnp.float32


def swap(x, r, n):
    if r == 0:
        return x
    return lax.ppermute(x, "sub", [(i, i ^ r) for i in range(n)])


def one_hot(mask):
    return jnp.where(mask, jnp.ones((), BF16), jnp.zeros((), BF16))


def by_group(groups, parts, shift):
    out = parts[shift % 4]
    for g in range(1, 4):
        out = jnp.where(groups == jnp.full((), g, groups.dtype), parts[(g + shift) % 4], out)
    return out


def iota(shape, dim):
    return lax.broadcasted_iota(jnp.int32, shape, dim)


def up_kernel(n_sub, cells, child_hbm, ops_hbm, partners_hbm, *refs):
    outs, refs = refs[:n_sub], refs[n_sub:]
    to_pair, to_other, child, ops, partners, sems = refs
    copies = [
        pltpu.make_async_copy(src, dst, sems.at[i])
        for i, (src, dst) in enumerate([(partners_hbm, partners), (child_hbm, child), (ops_hbm, ops)])
    ]
    for copy in copies:
        copy.start()
    order = child.shape[0]
    lane = iota((1, TILE), 1)
    row = iota((TILE, TILE), 0).astype(F32).astype(BF16)

    copies[0].wait()
    n_ops = partners.shape[0] // n_sub
    my_slab = lax.axis_index("slab")
    me = lax.axis_index("sub")
    for r in range(n_sub):
        q = me ^ r
        ids = partners[pl.ds(pl.multiple_of(q * n_ops, n_ops), n_ops), :]
        safe = jnp.maximum(ids, 0)
        source = lax.div(safe, cells)
        inner = safe - source * cells
        slab = lax.div(source, n_sub)
        block = (source - slab * n_sub) ^ q
        delta = slab - my_slab
        rim_at = n_sub * cells + block * (2 * RIM)
        column = jnp.where(
            delta == 0,
            block * cells + inner,
            jnp.where(delta < 0, rim_at + inner - (cells - RIM), rim_at + RIM + inner),
        )
        code = lax.shift_left(LANES + (column & (LANES - 1)), lax.shift_right_logical(column, 7))
        outs[r][order:, :] = jnp.where(ids >= 0, code, 0).astype(F32).astype(BF16)

    copies[1].wait()
    group = lax.shift_right_logical(lane, 5)
    chunks = []
    for q in range(4):
        want = 8 * (lane & (RIM - 1)) + 4 * lax.shift_right_logical(lane, 7) + ((group - q) & 3)
        hot = one_hot(row == jnp.broadcast_to(want.astype(F32).astype(BF16), (TILE, TILE)))
        chunk = jnp.dot(child[:, q * TILE : (q + 1) * TILE], hot, preferred_element_type=F32)
        chunks.append(chunk.astype(BF16))
    groups = jnp.broadcast_to(group[:, :LANES].astype(F32).astype(BF16), (order, LANES))
    copies[2].wait()
    total = None
    for j in range(4):
        turned = None
        for o in (j, j + 4):
            half = [x[:, o // 4 * LANES : (o // 4 + 1) * LANES] for x in chunks]
            part = jnp.dot(ops[o], by_group(groups, half, -j), preferred_element_type=F32)
            turned = part if turned is None else turned + part
        turned = turned if j == 0 else pltpu.roll(turned, LANES - RIM * j, 1)
        total = turned if total is None else total + turned
    total = total.astype(BF16)
    for r in range(n_sub):
        outs[r][:order, :] = total
    low, high = total[:, :RIM], total[:, cells - RIM :]
    even = lax.rem(my_slab, 2) == 0
    to_pair[...] = jnp.where(even, high, low)
    to_other[...] = jnp.where(even, low, high)


def up(child, ops, partners, n_sub):
    order = child.shape[0]
    cells = child.shape[1] // 8
    n_ops = partners.shape[0] // n_sub
    return pl.pallas_call(
        functools.partial(up_kernel, n_sub, cells),
        out_shape=[jax.ShapeDtypeStruct((order + n_ops, cells), BF16)] * n_sub
        + [jax.ShapeDtypeStruct((order, RIM), BF16)] * 2,
        in_specs=[HBM] * 3,
        out_specs=[VMEM] * (n_sub + 2),
        scratch_shapes=[
            pltpu.VMEM(child.shape, BF16),
            pltpu.VMEM(ops.shape, BF16),
            pltpu.VMEM(partners.shape, jnp.int32),
            pltpu.SemaphoreType.DMA((3,)),
        ],
        compiler_params=pltpu.CompilerParams(vmem_limit_bytes=16 << 20),
        cost_estimate=pl.CostEstimate(flops=1 << 30, bytes_accessed=2 << 20, transcendentals=0),
        name="up",
    )(*[pltpu.with_memory_space_constraint(x, pltpu.HBM) for x in (child, ops, partners)])


def spans_of(n_ops):
    return [(w, min(w + 32, n_ops)) for w in range(0, n_ops, 32)]


def pack(hit, n_ops):
    word = jnp.where(hit > 0.0, lax.shift_left(1, iota((n_ops, 1), 0) & 31), 0)
    return [jnp.sum(word[w:end]) for w, end in spans_of(n_ops)]


def each_bit(words, act, state):
    for i, word in enumerate(words):

        def step(carry, i=i):
            word, state = carry
            return word & (word - 1), act(32 * i + 31 - lax.clz(word & -word), state)

        state = lax.while_loop(lambda carry: carry[0] != 0, step, (word, state))[1]
    return state


def list_units(order, loads, n_ops, idx, code0, todo):
    cells = loads[0].shape[1]
    n_tiles = idx.shape[0]
    per = TILE // cells
    rows = iota((TILE, LANES), 0)
    code0[...] = lax.shift_left(LANES + (rows & (LANES - 1)), lax.shift_right_logical(rows, 7)).astype(F32).astype(BF16)
    hits = []
    for n in range(n_tiles):
        table = jnp.concatenate([x[order:, :].astype(F32) for x in loads[n * per : (n + 1) * per]], axis=1)
        idx[n, 0:n_ops, :] = table
        idx[n, n_ops : n_ops + 8, :] = jnp.zeros((8, TILE), F32)
        hits.append(jnp.max(table, axis=1, keepdims=True))
    count = jnp.int32(0)
    for n in range(n_tiles):

        def add(k, count, n=n):
            todo[count] = k * n_tiles + n
            return count + 1

        count = each_bit(pack(hits[n], n_ops), add, count)
    for a in range(GROUP):
        todo[count + a] = n_ops * n_tiles
    full = lax.div(count, GROUP)
    rest = count - full * GROUP
    short = jnp.logical_and(rest > 0, rest <= GROUP // 2)
    return jnp.where(rest > GROUP // 2, full + 1, full), short


def one_hots(row, base, first_tile, n_tiles):
    for t in range(first_tile, first_tile + n_tiles):
        scaled = (row * (4.0**-t)).astype(BF16)
        yield jnp.concatenate(
            [
                one_hot(base == jnp.broadcast_to(scaled[:, c : c + LANES], (TILE, LANES)))
                for c in range(0, TILE, LANES)
            ],
            axis=1,
        )


def pick_kernel(order, n_sub, *refs):
    loads, refs = refs[:n_sub], refs[n_sub:]
    ops_hbm, picked, ops, win, idx, code0, todo, sems = refs
    n_ops = ops.shape[0]
    n_tiles, k_tiles = idx.shape[0], win.shape[0]
    cells = loads[0].shape[1]
    cuts = [i * n_ops // FETCHES for i in range(FETCHES + 1)]
    copies = [
        pltpu.make_async_copy(ops_hbm.at[a:b], ops.at[a:b], sems.at[i]) for i, (a, b) in enumerate(zip(cuts, cuts[1:]))
    ]
    for copy in copies:
        copy.start()
    for r in range(n_sub):
        win[r * cells // TILE, :, r * cells % TILE : r * cells % TILE + cells] = loads[r][:order, :]
    full, short = list_units(order, loads, n_ops, idx, code0, todo)

    def gather(i, size):
        base = code0[...]
        for a in range(size):
            u = todo[GROUP * i + a]
            k = lax.div(u, n_tiles)
            row = idx[u - k * n_tiles, pl.ds(k, 1), :]
            total = None
            for t, hot in enumerate(one_hots(row, base, 0, k_tiles)):
                part = jnp.dot(win[t], hot, preferred_element_type=F32)
                total = part if total is None else total + part
            picked[GROUP * i + a] = total.astype(BF16)

    def body(i, carry):
        gather(i, GROUP)
        return carry

    lax.fori_loop(0, full, body, 0)

    @pl.when(short)
    def _():
        gather(full, GROUP // 2)

    for copy in copies:
        copy.wait()


def apply_kernel(order, n_sub, *refs):
    loads, sides, refs = refs[:n_sub], refs[n_sub : 2 * n_sub], refs[2 * n_sub :]
    picked, ops, refs = refs[0], refs[1], refs[2:]
    outs, (win, idx, code0, acc, cols, todo) = refs[:n_sub], refs[n_sub:]
    n_ops = ops.shape[0]
    n_tiles, k_tiles = idx.shape[0], win.shape[0]
    cells = loads[0].shape[1]
    for i in range(0, n_sub, 2):
        at = i // 2 * LANES
        pair = jnp.concatenate([sides[i][...], sides[i + 1][...]], axis=1)
        win[at // TILE, :, at % TILE : at % TILE + LANES] = pair
    full, short = list_units(order, loads, n_ops, idx, code0, todo)
    acc[...] = jnp.zeros_like(acc)

    def gather(i, size):
        base = code0[...]
        for a in range(size):
            u = todo[GROUP * i + a]
            k = lax.div(u, n_tiles)
            row = idx[u - k * n_tiles, pl.ds(k, 1), :]
            total = None
            for t, hot in enumerate(one_hots(row, base, n_sub * cells // TILE, k_tiles)):
                part = jnp.dot(win[t], hot, preferred_element_type=F32)
                total = part if total is None else total + part
            cols[i & 1, a] = total.astype(BF16) + picked[GROUP * i + a]

    def apply(i, size):
        for a in range(size):
            u = todo[GROUP * i + a]
            k = lax.div(u, n_tiles)
            acc[u - k * n_tiles] += jnp.dot(
                ops[jnp.minimum(k, n_ops - 1)], cols[i & 1, a], preferred_element_type=F32
            )

    def body(i, carry):
        apply(i - 1, GROUP)
        gather(i, GROUP)
        return carry

    @pl.when(full > 0)
    def _():
        gather(0, GROUP)
        lax.fori_loop(1, full, body, 0)

    @pl.when(jnp.logical_and(full > 0, jnp.logical_not(short)))
    def _():
        apply(full - 1, GROUP)

    @pl.when(jnp.logical_and(full > 0, short))
    def _():
        apply(full - 1, GROUP)
        gather(full, GROUP // 2)

    @pl.when(jnp.logical_and(full == 0, short))
    def _():
        gather(full, GROUP // 2)

    @pl.when(short)
    def _():
        apply(full, GROUP // 2)

    for j, out in enumerate(outs):
        out[...] = acc[j * cells // TILE, :, j * cells % TILE : j * cells % TILE + cells].astype(out.dtype)


def m2l_sizes(loads, ops):
    n_sub, cells = len(loads), loads[0].shape[1]
    n_tiles = n_sub * cells // TILE
    return n_sub, cells, n_tiles, ops.shape[0] * n_tiles + GROUP


def pick(loads, ops, order):
    n_sub, cells, n_tiles, units = m2l_sizes(loads, ops)
    n_ops = ops.shape[0]
    return pl.pallas_call(
        functools.partial(pick_kernel, order, n_sub),
        out_shape=[jax.ShapeDtypeStruct((units, order, TILE), BF16), jax.ShapeDtypeStruct(ops.shape, BF16)],
        in_specs=[VMEM] * n_sub + [HBM],
        out_specs=[VMEM] * 2,
        scratch_shapes=[
            pltpu.VMEM((n_sub * cells // TILE, order, TILE), BF16),
            pltpu.VMEM((n_tiles, n_ops + 8, TILE), F32),
            pltpu.VMEM((TILE, LANES), BF16),
            pltpu.SMEM((units,), jnp.int32),
            pltpu.SemaphoreType.DMA((FETCHES,)),
        ],
        compiler_params=pltpu.CompilerParams(vmem_limit_bytes=24 << 20),
        cost_estimate=pl.CostEstimate(flops=4 << 30, bytes_accessed=4 << 20, transcendentals=0),
        name="pick",
    )(*loads, pltpu.with_memory_space_constraint(ops, pltpu.HBM))


def apply_ops(loads, sides, picked, ops, order):
    n_sub, cells, n_tiles, units = m2l_sizes(loads, ops)
    n_ops = ops.shape[0]
    return pl.pallas_call(
        functools.partial(apply_kernel, order, n_sub),
        out_shape=[jax.ShapeDtypeStruct((order, cells), F32 if r == 0 else BF16) for r in range(n_sub)],
        in_specs=[VMEM] * (2 * n_sub + 2),
        out_specs=[VMEM] * n_sub,
        scratch_shapes=[
            pltpu.VMEM((n_sub * 2 * RIM // TILE, order, TILE), BF16),
            pltpu.VMEM((n_tiles, n_ops + 8, TILE), F32),
            pltpu.VMEM((TILE, LANES), BF16),
            pltpu.VMEM((n_tiles, order, TILE), F32),
            pltpu.VMEM((2, GROUP, order, TILE), BF16),
            pltpu.SMEM((units,), jnp.int32),
        ],
        compiler_params=pltpu.CompilerParams(vmem_limit_bytes=24 << 20),
        cost_estimate=pl.CostEstimate(flops=4 << 30, bytes_accessed=4 << 20, transcendentals=0),
        name="apply",
    )(*loads, *sides, picked, ops)


def down_kernel(n_parts, incoming, *refs):
    parts = refs[:n_parts]
    ops, out, stage, sem = refs[n_parts:]
    cells = incoming.shape[1]
    far = parts[0][...].astype(F32)
    for r in range(1, n_parts):
        far = far + parts[r][...].astype(F32)
    held = (incoming[...].astype(F32) + far).astype(BF16)
    order = held.shape[0]
    lane = iota((1, TILE), 1)
    row = iota((TILE, LANES), 0)
    base = 8 * (row & (RIM - 1)) + 4 * lax.shift_right_logical(row, 7)
    quarter = lax.shift_right_logical(row, 5)
    lane16 = lane.astype(F32).astype(BF16)
    groups = jnp.broadcast_to(lax.shift_right_logical(lane[:, :LANES], 5), (order, LANES))
    wide = held.astype(F32)
    turned = [held] + [pltpu.roll(wide, RIM * j, 1).astype(BF16) for j in range(1, 4)]
    made = [jnp.dot(ops[o], turned[o % 4], preferred_element_type=F32) for o in range(8)]
    copies = []
    for q in range(8 * cells // TILE):
        have = (base + ((quarter - q) & 3)).astype(F32).astype(BF16)
        hot = jnp.concatenate(
            [one_hot(have == jnp.broadcast_to(lane16[:, c : c + LANES], (TILE, LANES))) for c in (0, LANES)], axis=1
        )
        rest = jnp.concatenate([by_group(groups, made[4 * h : 4 * h + 4], -q) for h in range(2)], axis=1)
        total = None
        for _ in range(2):
            top = rest.astype(BF16)
            part = jnp.dot(top, hot, preferred_element_type=F32)
            total = part if total is None else total + part
            rest = rest - top.astype(F32)
        stage[q] = total
        copy = pltpu.make_async_copy(stage.at[q], out.at[:, q * TILE : (q + 1) * TILE], sem.at[q])
        copy.start()
        copies.append(copy)
    for copy in copies:
        copy.wait()


def down(incoming, parts, ops):
    order, cells = incoming.shape
    chunks = 8 * cells // TILE
    return pl.pallas_call(
        functools.partial(down_kernel, len(parts)),
        out_shape=jax.ShapeDtypeStruct((order, 8 * cells), F32),
        in_specs=[VMEM] * (len(parts) + 2),
        out_specs=pl.BlockSpec(memory_space=pl.ANY),
        scratch_shapes=[pltpu.VMEM((chunks, order, TILE), F32), pltpu.SemaphoreType.DMA((chunks,))],
        compiler_params=pltpu.CompilerParams(vmem_limit_bytes=16 << 20),
        cost_estimate=pl.CostEstimate(flops=1 << 30, bytes_accessed=2 << 20, transcendentals=0),
        name="down",
    )(incoming, *parts, ops)


def far_field(child_moments, incoming, m2m_ops, m2l_ops, l2l_ops, partners):
    order, cells = incoming.shape
    n_sub = lax.axis_size("sub")
    n_slab = lax.axis_size("slab")
    assert n_sub & (n_sub - 1) == 0 and n_slab % 2 == 0 and cells == LANES == 4 * RIM
    *sends, to_pair, to_other = up(child_moments, m2m_ops, partners, n_sub)
    got_pair = lax.ppermute(to_pair, "slab", [(i, i ^ 1) for i in range(n_slab)])
    got_other = lax.ppermute(to_other, "slab", [(i, ((i + 1) ^ 1) - 1) for i in range(1, n_slab - 1)])
    loads = [swap(sends[r], r, n_sub) for r in range(n_sub)]
    even = lax.axis_index("slab") % 2 == 0
    rim = jnp.concatenate(
        [jnp.where(even, got_other, got_pair), jnp.where(even, got_pair, got_other)], axis=1
    )
    sides = [swap(rim, r, n_sub) for r in range(n_sub)]
    picked, held_ops = pick(loads, m2l_ops, order)
    mine, *others = apply_ops(loads, sides, picked, held_ops, order)
    back = [swap(x, r + 1, n_sub) for r, x in reversed(list(enumerate(others)))]
    return down(incoming, [mine, *back], l2l_ops)


def solution(mesh):
    in_specs = (
        P(None, ("slab", "sub")),
        P(None, ("slab", "sub")),
        P(),
        P("sub", None, None),
        P(),
        P(None, ("slab", "sub")),
    )
    out_specs = P(None, ("slab", "sub"))
    return jax.shard_map(far_field, mesh=mesh, in_specs=in_specs, out_specs=out_specs, check_vma=False)
```
